256 devices in a mesh: gx: 8 (over z_lo, x), gy: 4 (over z_hi), gz: 8 (over y, core).
Axes of the slice: x: 4, y: 4, z: 8 (z_hi: 4, z_lo: 2; z = z_hi * 2 + z_lo), core: 2. Of those that a mesh axis runs over, the one named last changes fastest.
Arguments:
- displacement: bfloat16 [3, 32, 128, 128], P(None, 'gx', 'gy', 'gz'), may hold values from -6 to 6
- lift_weight: bfloat16 [27, 64, 3], replicated, may hold values from -1 to 1
- encode_weight: bfloat16 [27, 64, 64], replicated, may hold values from -0.21875 to 0.21875
- downward_weight: bfloat16 [8, 128, 64], replicated, may hold values from -0.375 to 0.375
- middle_first: bfloat16 [27, 128, 128], replicated, may hold values from -0.15625 to 0.15625
- middle_second: bfloat16 [27, 128, 128], replicated, may hold values from -0.15625 to 0.15625
- up_weight: bfloat16 [8, 64, 128], replicated, may hold values from -0.75 to 0.75
- decode_weight: bfloat16 [27, 64, 128], replicated, may hold values from -0.15625 to 0.15625
- head_weight: bfloat16 [3, 64], replicated, may hold values from -1 to 1
Outputs:
- imitated: float32 [3, 32, 128, 128], P(None, 'gx', 'gy', 'gz')
The draws below stay inside these ranges and needn't reach their ends.
All inputs are finite; a program needn't handle non-finite values.
Results may differ from the reference program's by a relative error of at most 0.0055.
Values may be sent and summed in bfloat16 or wider, within the bound.
No kernel may reach another device: no remote copies, remote signals or barrier semaphores. Data moves between devices by JAX's collectives and lax.ppermute only.
A program may use at most 64 MiB of HBM per device.

```python
import jax
import jax.numpy as jnp

C1 = 64
C2 = 128
NX = 32
NY = 128
NZ = 128


def levels(stream_key, shape, pieces, low, top_value):
    loudness, own = 1.0, jax.random.fold_in(stream_key, 6)
    for position, parts in pieces:
        steps = jnp.exp(jax.random.uniform(jax.random.fold_in(own, position), (parts,), jnp.float32, low / len(pieces), top_value / len(pieces)))
        loudness = loudness * jnp.repeat(steps, shape[position] // parts).reshape([-1 if axis == position else 1 for axis in range(len(shape))])
    return loudness


def noise(stream_key, shape, scale, bound, shards=(), kind=jnp.bfloat16):
    entries = jax.random.normal(stream_key, shape, jnp.float32) * scale
    if len(shards) > 0:
        entries = levels(stream_key, shape, shards, -0.22, 0.18) * entries
    return jnp.clip(entries, min=-bound, max=bound).astype(kind)


def setup_inputs(seed: int = 0) -> dict:
    streams_of = jax.random.split(jax.random.key(seed), 10)
    return {
        "displacement": noise(streams_of[0], (3, NX, NY, NZ), 1.0, 6.0, ((1, 8), (2, 4), (3, 8))),
        "lift_weight": noise(streams_of[1], (27, C1, 3), (81 // 2) ** -0.5, 1.0),
        "encode_weight": noise(streams_of[2], (27, C1, C1), (27 * C1 // 2) ** -0.5, 0.21875),
        "downward_weight": noise(streams_of[3], (8, C2, C1), (4 * C1) ** -0.5, 0.375),
        "middle_first": noise(streams_of[4], (27, C2, C2), (27 * C2 // 2) ** -0.5, 0.15625),
        "middle_second": noise(streams_of[5], (27, C2, C2), (27 * C2 // 2) ** -0.5, 0.15625),
        "up_weight": noise(streams_of[6], (8, C1, C2), (C2 // 2) ** -0.5, 0.75),
        "decode_weight": noise(streams_of[7], (27, C1, 2 * C1), (27 * C1) ** -0.5, 0.15625),
        "head_weight": noise(streams_of[8], (3, C1), (C1 // 2) ** -0.5, 1.0),
    }


def apply_relu(value):
    return jnp.where(value > 0, value, 0.1 * value)


def conv_periodic(field, weight_tensor):
    padded = jnp.pad(field, ((0, 0), (1, 1), (1, 1), (1, 1)), mode="wrap")
    size_x, size_y, size_z = field.shape[1], field.shape[2], field.shape[3]
    weights32 = weight_tensor.astype(jnp.float32)
    summed = jnp.zeros((weight_tensor.shape[1], size_x, size_y, size_z), jnp.float32)
    for offset in range(27):
        a, b, c = offset // 9, (offset // 3) % 3, offset % 3
        window = padded[:, a:a + size_x, b:b + size_y, c:c + size_z].astype(jnp.float32)
        summed = summed + jnp.einsum("oi,ixyz->oxyz", weights32[offset], window)
    return summed


def reduce_resolution(fine_level, weight_tensor):
    chans, size_x, size_y, size_z = fine_level.shape
    blocks = fine_level.reshape(chans, size_x // 2, 2, size_y // 2, 2, size_z // 2, 2).astype(jnp.float32)
    kernel = weight_tensor.reshape(2, 2, 2, weight_tensor.shape[1], weight_tensor.shape[2]).astype(jnp.float32)
    return jnp.einsum("abcoi,ixaybzc->oxyz", kernel, blocks)


def upsample(coarse_field, weight_tensor):
    chans, size_x, size_y, size_z = coarse_field.shape
    kernel = weight_tensor.reshape(2, 2, 2, weight_tensor.shape[1], weight_tensor.shape[2]).astype(jnp.float32)
    result = jnp.einsum("abcoi,ixyz->oxaybzc", kernel, coarse_field.astype(jnp.float32))
    return result.reshape(weight_tensor.shape[1], 2 * size_x, 2 * size_y, 2 * size_z)


def reference(displacement, lift_weight, encode_weight, downward_weight, middle_first, middle_second, up_weight, decode_weight, head_weight):
    first = apply_relu(conv_periodic(displacement, lift_weight)).astype(jnp.bfloat16)
    skip_link = apply_relu(conv_periodic(first, encode_weight)).astype(jnp.bfloat16)
    coarse_level = apply_relu(reduce_resolution(skip_link, downward_weight)).astype(jnp.bfloat16)
    middle = apply_relu(conv_periodic(coarse_level, middle_first)).astype(jnp.bfloat16)
    deep = apply_relu(conv_periodic(middle, middle_second)).astype(jnp.bfloat16)
    upsampled = apply_relu(upsample(deep, up_weight)).astype(jnp.bfloat16)
    stacked = jnp.concatenate([skip_link, upsampled], axis=0)
    joined = apply_relu(conv_periodic(stacked, decode_weight)).astype(jnp.bfloat16)
    head = jnp.einsum("oi,ixyz->oxyz", head_weight.astype(jnp.float32), joined.astype(jnp.float32))
    return displacement.astype(jnp.float32) + head
```

```python
import jax
import jax.numpy as jnp
import numpy as np
from jax import lax
from jax.experimental import pallas as pl
from jax.experimental.pallas import tpu as pltpu
from jax.sharding import PartitionSpec as P

BF, F32 = jnp.bfloat16, jnp.float32


def shift(block, axis, step):
    count = lax.axis_size(axis)
    return lax.ppermute(block, axis, [(i, (i + step) % count) for i in range(count)])


def act(value):
    return jnp.maximum(value, 0.1 * value)


def picker():
    table = np.zeros((3, 128, 8, 128), np.float32)
    for b in range(3):
        for q in range(8):
            for a in range(2):
                for ch in range(3):
                    for zi in range(6):
                        z = 4 * q + zi - 1
                        if 0 <= z < 32:
                            row = 48 + 8 * ch + z if z < 8 else 16 * ch + z - 8 if z < 24 else 48 + 8 * ch + z
                            table[b, row, q, 18 * (3 * a + b) + 6 * ch + zi] = 1
    return table.reshape(384, 1024)


def lift_matrix(w):
    w = jnp.transpose(w.reshape(9, 3, 64, 3), (0, 3, 1, 2))
    cols = [jnp.pad(w, ((0, 0), (0, 0), (zo, 3 - zo), (0, 0))) for zo in range(4)]
    m = jnp.concatenate(cols, axis=3).reshape(162, 256)
    return jnp.concatenate([m[:108], jnp.zeros((20, 256), BF), m[108:], jnp.zeros((74, 256), BF)], axis=0)


def quad_matrix(w):
    t = jnp.swapaxes(w, 1, 2).reshape(9, 3, w.shape[2], 64)
    c0, c1, c2 = t[:, 0], t[:, 1], t[:, 2]
    o = jnp.zeros_like(c0)
    cols = [[c1, c2, o, o, o, c0], [c0, c1, c2, o, o, o], [o, c0, c1, c2, o, o], [o, o, c0, c1, c2, o]]
    return jnp.concatenate([jnp.concatenate(c, axis=1) for c in cols], axis=2)


def pair_matrix(w):
    t = jnp.swapaxes(w, 1, 2).reshape(9, 3, 128, 128)
    c0, c1, c2 = t[:, 0], t[:, 1], t[:, 2]
    o = jnp.zeros_like(c0)
    cols = [[c0, c1, c2, o], [o, c0, c1, c2]]
    return jnp.concatenate([jnp.concatenate(c, axis=1) for c in cols], axis=2)


def head_matrix(w):
    wt = w.T
    m = jnp.einsum("zs,ck->zcks", jnp.eye(16, dtype=BF), wt)
    return jnp.pad(m.reshape(1024, 48), ((0, 0), (0, 80)))


def weights(lift, encode, down, m1, m2, up, decode, head):
    we = quad_matrix(encode).reshape(3456, 256)
    ws, wu = quad_matrix(decode[:, :, :64]), quad_matrix(decode[:, :, 64:])
    wdec = jnp.concatenate([ws, wu], axis=1).reshape(6912, 256)
    return (
        lift_matrix(lift), we, jnp.swapaxes(down, 1, 2).reshape(512, 128),
        pair_matrix(m1).reshape(4608, 256), pair_matrix(m2).reshape(4608, 256),
        jnp.transpose(up, (2, 0, 1)).reshape(128, 512), wdec, head_matrix(head),
    )


def dot(a, b):
    return jnp.dot(a, b, preferred_element_type=F32)


def rows(parts):
    flat = [p.reshape(-1, p.shape[-1]) for p in parts]
    return flat[0] if len(flat) == 1 else jnp.concatenate(flat, axis=1)


def up_one(v):
    return pltpu.roll(v, v.shape[-2] - 1, v.ndim - 2)


def kernel(d_ref, s_ref, wl_ref, we_ref, wd_ref, w1_ref, w2_ref, wu_ref, wdec_ref, wh_ref, o_ref,
           dt, db, fp, fe, sk, sd, c1, c2, de, uu, es, eu):
    for yo in range(8):
        for xo in range(12):
            t = [d_ref[pl.ds((8 * xi + xo) * 48 + yo, 8, stride=6), :] for xi in range(2)]
            dt[yo, xo] = jnp.concatenate(t, axis=0).astype(BF)

    lane = lax.broadcasted_iota(jnp.int32, (16, 128), 1)
    first_slots = lane < 54
    low = lane < 64

    for h in range(4):
        r = dot(rows([dt[b:b + 6] for b in range(3)]), s_ref[:, 256 * h:256 * h + 256])
        r = r.astype(BF).reshape(6, 12, 16, 256)
        db[2 * h] = r[..., :128]
        db[2 * h + 1] = r[..., 128:]

    def lift_step(q, carry):
        for g in range(2):
            y = slice(3 * g, 3 * g + 3)
            ta = jnp.where(first_slots, db[q, y, 0:10], db[q, y, 1:11])
            r = act(dot(rows([ta, db[q, y, 2:12]]), wl_ref[...]))
            for half in range(2):
                part = r[:, 128 * half:128 * half + 128].reshape(3, 10, 16, 128)
                fp[2 * q + half, y] = part.astype(BF)
                if g == 0:
                    low_rows = part[0:2].reshape(40, 8, 128)
                    fp[2 * q + half, 6:8] = up_one(low_rows).reshape(2, 10, 16, 128).astype(BF)
        return carry

    lax.fori_loop(0, 8, lift_step, 0)

    def edge_step(q, carry):
        fe[q] = jnp.where(low, fp[2 * q + 3], fp[2 * q])
        return carry

    lax.fori_loop(0, 7, edge_step, 0)

    def encode_step(q, carry):
        for g in range(2):
            y0 = 3 * g
            acc = None
            for lo, hi in ((0, 2), (2, 4), (4, 6), (6, 9)):
                parts = []
                for t in range(lo, hi):
                    a, b = t // 3, t % 3
                    sl = (slice(y0 + b, y0 + b + 3), slice(a, a + 8))
                    parts += [fp[(2 * q + 1,) + sl], fp[(2 * q + 2,) + sl], fe[(q,) + sl]]
                p = dot(rows(parts), we_ref[384 * lo:384 * hi, :])
                acc = p if acc is None else acc + p
            r = act(acc).reshape(3, 8, 2, 8, 256)
            for half in range(2):
                part = r[..., 128 * half:128 * half + 128]
                packed = part.reshape(3, 8, 16, 128).astype(BF)
                sp = 2 * q + half
                for yy in range(3):
                    yo = y0 + yy
                    sk[sp, yo // 2, yo % 2] = packed[yy].reshape(4, 2, 16, 128)
                    mixed = [jnp.concatenate([part[yy, 5 + xo, 0] if 5 + xo < 8 else part[yy, 5 + xo - 8, 1],
                                              part[yy, 7 + xo, 0] if 7 + xo < 8 else part[yy, 7 + xo - 8, 1]], axis=0)
                             for xo in range(4)]
                    mixed = jnp.stack(mixed).reshape(8, 8, 128)
                    if yo == 5:
                        sd[sp, 0] = mixed.reshape(4, 16, 128).astype(BF)
                    moved = up_one(mixed)
                    sd[sp, yo + 1] = moved.reshape(4, 16, 128).astype(BF)
                    if yo == 0:
                        sd[sp, 7] = up_one(moved).reshape(4, 16, 128).astype(BF)
        return carry

    lax.fori_loop(0, 7, encode_step, 0)

    r = act(dot(rows([sk[:, :, b, :, a] for a in range(2) for b in range(2)]), wd_ref[...]))
    r = r.reshape(7, 2, 3, 4, 2, 8, 128)
    for yo in range(3):
        for xo in range(5):
            t = jnp.stack([r[:, :, yo, xo % 4, xo // 4], r[:, :, yo, (3 + xo) % 4, (3 + xo) // 4]], axis=2)
            c1[:, :, yo, xo] = t.reshape(7, 2, 16, 128).astype(BF)
            if yo < 2:
                c1[:, :, yo + 3, xo] = up_one(t.reshape(28, 8, 128)).reshape(7, 2, 16, 128).astype(BF)

    def middle(src, w_ref, zp, xn):
        acc = None
        for t in range(9):
            a, b = t // 3, t % 3
            parts = [src[zi // 2:zi // 2 + zp, zi % 2, b:b + 3, a:a + xn] for zi in range(4)]
            p = dot(rows(parts), w_ref[512 * t:512 * t + 512, :])
            acc = p if acc is None else acc + p
        return act(acc).reshape(zp, 3, xn, 2, 8, 256)

    r = middle(c1, w1_ref, 6, 3)
    for half in range(2):
        part = r[..., 128 * half:128 * half + 128]
        for yo in range(3):
            for xo in range(4):
                t = jnp.stack([part[:, yo, xo % 3, xo // 3], part[:, yo, (2 + xo) % 3, (2 + xo) // 3]], axis=1)
                c2[:, half, yo, xo] = t.reshape(6, 16, 128).astype(BF)
                if yo < 2:
                    c2[:, half, yo + 3, xo] = up_one(t.reshape(12, 8, 128)).reshape(6, 16, 128).astype(BF)

    r = middle(c2, w2_ref, 5, 2).reshape(5, 3, 2, 16, 256).astype(BF)
    de[:, 0] = r[..., :128]
    de[:, 1] = r[..., 128:]

    r = act(dot(rows([de[...]]), wu_ref[...])).reshape(5, 2, 3, 2, 2, 8, 512)
    for yo in range(6):
        b = yo % 2
        for xo in range(4):
            t = []
            for f in (1 + xo, 3 + xo):
                a = f % 2
                n = 128 * (2 * a + b)
                t.append(r[:, :, yo // 2, (f // 2) % 2, f // 4, :, n:n + 128])
            t = jnp.stack(t, axis=2)
            if yo > 0:
                uu[:, :, yo - 1, xo] = t.reshape(5, 2, 16, 128).astype(BF)
            if yo < 3:
                uu[:, :, yo + 5, xo] = up_one(t.reshape(20, 8, 128)).reshape(5, 2, 16, 128).astype(BF)

    for q in range(4):
        es[q] = jnp.where(low, sd[2 * q + 5], sd[2 * q + 2])
        eu[q] = jnp.where(low, uu[q + 1, 1], uu[q, 0])

    for g in range(1):
        acc = None
        for t in range(9):
            a, b = t // 3, t % 3
            ys, xs = slice(b, b + 6), slice(a, a + 2)
            own = [jnp.stack([sd[2 * q + 3 + k, ys, xs] for q in range(4)]) for k in range(2)]
            parts = own + [es[:, ys, xs], uu[0:4, 1, ys, xs], uu[1:5, 0, ys, xs], eu[:, ys, xs]]
            p = dot(rows(parts), wdec_ref[768 * t:768 * t + 768, :])
            acc = p if acc is None else acc + p
        j = act(acc).astype(BF).reshape(4, 192, 256)
        o_ref[...] = dot(jnp.concatenate([j[q] for q in range(4)], axis=1), wh_ref[...])


def compute(d, ws):
    flat = jnp.pad(d.astype(F32).reshape(960, 96), ((0, 8), (0, 32)))
    V = pltpu.VMEM
    out = pl.pallas_call(
        kernel,
        out_shape=jax.ShapeDtypeStruct((192, 128), F32),
        in_specs=[pl.BlockSpec(memory_space=pltpu.VMEM)] * 10,
        out_specs=pl.BlockSpec(memory_space=pltpu.VMEM),
        scratch_shapes=[
            V((8, 12, 16, 128), BF), V((8, 6, 12, 16, 128), BF), V((16, 8, 10, 16, 128), BF), V((7, 8, 10, 16, 128), BF),
            V((14, 3, 2, 4, 2, 16, 128), BF), V((14, 8, 4, 16, 128), BF), V((7, 2, 5, 5, 16, 128), BF),
            V((6, 2, 5, 4, 16, 128), BF), V((5, 2, 3, 2, 16, 128), BF), V((5, 2, 8, 4, 16, 128), BF),
            V((4, 8, 4, 16, 128), BF), V((4, 8, 4, 16, 128), BF),
        ],
        compiler_params=pltpu.CompilerParams(vmem_limit_bytes=60 << 20),
        cost_estimate=pl.CostEstimate(flops=20_000_000_000, bytes_accessed=20_000_000, transcendentals=0),
    )(flat, jnp.asarray(picker(), BF), *ws)
    out = out[:, :48].reshape(6, 2, 2, 8, 3, 16)
    return jnp.transpose(out, (4, 2, 1, 3, 0, 5)).reshape(3, 4, 48, 16)[:, :, :32]


def local(displacement, *raw):
    ws = weights(*raw)
    d = jnp.concatenate([displacement[0], displacement[1], displacement[2]], axis=-1)
    d = jnp.concatenate([shift(d, "gx", 2), shift(d, "gx", 1), d, shift(d, "gx", -1), shift(d, "gx", -2)], axis=0)
    d = jnp.concatenate([shift(d[:, 24:], "gy", 1), d, shift(d[:, :8], "gy", -1)], axis=1)
    left = jnp.concatenate([d[..., 16 * k + 8:16 * k + 16] for k in range(3)], axis=-1)
    right = jnp.concatenate([d[..., 16 * k:16 * k + 8] for k in range(3)], axis=-1)
    d = jnp.concatenate([d, shift(left, "gz", 1), shift(right, "gz", -1)], axis=-1)
    return displacement.astype(F32) + compute(d, ws)


def solution(mesh):
    placed = (P(None, "gx", "gy", "gz"), P(), P(), P(), P(), P(), P(), P(), P())
    return jax.shard_map(local, mesh=mesh, in_specs=placed, out_specs=P(None, "gx", "gy", "gz"), check_vma=False)
```

```python
import jax
import jax.numpy as jnp
import numpy as np
from jax import lax
from jax.experimental import pallas as pl
from jax.experimental.pallas import tpu as pltpu
from jax.sharding import PartitionSpec as P

BF, F32 = jnp.bfloat16, jnp.float32


def shift(block, axis, step):
    count = lax.axis_size(axis)
    return lax.ppermute(block, axis, [(i, (i + step) % count) for i in range(count)])


def act(value):
    return jnp.maximum(value, 0.1 * value)


def picker():
    table = np.zeros((3, 128, 8, 128), np.float32)
    for b in range(3):
        for q in range(8):
            for a in range(2):
                for ch in range(3):
                    for zi in range(6):
                        z = 4 * q + zi - 1
                        if 0 <= z < 32:
                            start = (48, 24 - 8, -16, 72 - 24)[z // 8]
                            table[b, start + 8 * ch + z, q, 18 * (3 * a + b) + 6 * ch + zi] = 1
    return table.reshape(384, 1024)


def lift_matrix(w):
    w = jnp.transpose(w.reshape(9, 3, 64, 3), (0, 3, 1, 2))
    cols = [jnp.pad(w, ((0, 0), (0, 0), (zo, 3 - zo), (0, 0))) for zo in range(4)]
    m = jnp.concatenate(cols, axis=3).reshape(162, 256)
    return jnp.concatenate([m[:108], jnp.zeros((20, 256), BF), m[108:], jnp.zeros((74, 256), BF)], axis=0)


def head_matrix(w):
    wt = w.T
    m = jnp.einsum("zs,ck->zcks", jnp.eye(16, dtype=BF), wt)
    return jnp.pad(m.reshape(1024, 48), ((0, 0), (0, 80)))


def banded_kernel(e_ref, d_ref, m1_ref, m2_ref, u_ref, j_ref, we, wd, w1, w2, wu, wj):
    def turned(value):
        return jnp.transpose(value.astype(F32)).astype(BF)

    def quad(raw, t, width):
        c = [raw[3 * t + k] for k in range(3)]
        o = jnp.zeros_like(c[0])
        blocks = [turned(jnp.concatenate(p, axis=0)) for p in ((c[0], o), (c[1], c[0]), (c[2], c[1]), (o, c[2]))]
        empty = jnp.zeros((width, 128), BF)
        order = (0, 1, 2, 3, 4, -1)
        return [[blocks[z - 2 * p + 1] if 0 <= z - 2 * p + 1 < 4 else empty for z in order] for p in range(2)]

    def step(t, carry):
        for p, column in enumerate(quad(e_ref, t, 64)):
            for k, block in enumerate(column):
                we[t, 64 * k:64 * k + 64, 128 * p:128 * p + 128] = block
        for p, column in enumerate(quad(j_ref, t, 128)):
            for k, block in enumerate(column):
                wj[t, 64 * k:64 * k + 64, 128 * p:128 * p + 128] = block[:64]
                wj[t, 384 + 64 * k:448 + 64 * k, 128 * p:128 * p + 128] = block[64:]
        for raw, out in ((m1_ref, w1), (m2_ref, w2)):
            c = [turned(raw[3 * t + k]) for k in range(3)]
            empty = jnp.zeros((128, 128), BF)
            for zo in range(2):
                for zi in range(4):
                    out[t, 128 * zi:128 * zi + 128, 128 * zo:128 * zo + 128] = c[zi - zo] if 0 <= zi - zo < 3 else empty
        return carry

    lax.fori_loop(0, 9, step, 0)
    for k in range(4):
        wd[128 * k:128 * k + 64] = turned(d_ref[2 * k])
        wd[128 * k + 64:128 * k + 128] = turned(d_ref[2 * k + 1])
        wu[:, 128 * k:128 * k + 128] = turned(jnp.concatenate([u_ref[2 * k], u_ref[2 * k + 1]], axis=0))


def weights(lift, encode, down, m1, m2, up, decode, head):
    shapes = ((9, 384, 256), (512, 128), (9, 512, 256), (9, 512, 256), (128, 512), (9, 768, 256))
    we, wd, w1, w2, wu, wj = pl.pallas_call(
        banded_kernel,
        out_shape=[jax.ShapeDtypeStruct(shape, BF) for shape in shapes],
        in_specs=[pl.BlockSpec(memory_space=pltpu.VMEM)] * 6,
        out_specs=[pl.BlockSpec(memory_space=pltpu.VMEM)] * 6,
        compiler_params=pltpu.CompilerParams(vmem_limit_bytes=40 << 20),
        cost_estimate=pl.CostEstimate(flops=5_000_000_000, bytes_accessed=14_000_000, transcendentals=0),
    )(encode, down, m1, m2, up, decode)
    return (
        lift_matrix(lift), we.reshape(3456, 256), wd, w1.reshape(4608, 256), w2.reshape(4608, 256),
        wu, wj.reshape(6912, 256), head_matrix(head),
    )


def dot(a, b):
    return jnp.dot(a, b, preferred_element_type=F32)


def rows(parts):
    flat = [p.reshape(-1, p.shape[-1]) for p in parts]
    return flat[0] if len(flat) == 1 else jnp.concatenate(flat, axis=1)


def up_one(v):
    return pltpu.roll(v, v.shape[-2] - 1, v.ndim - 2)


def plane_kernel(d_ref, a_ref, top_ref, low_ref):
    for x in range(4):
        parts = [d_ref[k, x].astype(F32)[h:h + 8] for h in (8, 0) for k in range(3)]
        t = jnp.transpose(jnp.concatenate(parts, axis=0))
        t = jnp.concatenate([t, jnp.zeros((32, 80), F32)], axis=1)
        a_ref[x] = t.astype(BF)
        top_ref[x] = t[24:].astype(BF)
        low_ref[x] = t[:8].astype(BF)


def join_kernel(before_ref, a_ref, after_ref, o_ref):
    for x in range(4):
        parts = [r[x].astype(F32) for r in (before_ref, a_ref, after_ref)]
        o_ref[x] = jnp.concatenate(parts, axis=0).astype(BF)


def rim_kernel(b0, b1, b2, b3, b4, left_ref, right_ref):
    lane = lax.broadcasted_iota(jnp.int32, (16, 128), 1)
    for x in range(20):
        own = (b0, b1, b2, b3, b4)[x // 4][x % 4].astype(F32)
        for out, first in ((left_ref, 0), (right_ref, 24)):
            g = [own[16 * k:16 * k + 16] for k in range(3)]
            g = [t if 24 * k == first else pltpu.roll(t, (24 * k - first) % 128, 1) for k, t in enumerate(g)]
            out[x] = jnp.where(lane < 24, g[0], jnp.where(lane < 48, g[1], g[2])).astype(BF)


def tiles(df, dt):
    for yo in range(8):
        for xo in range(12):
            t = [df[pl.ds((8 * xi + xo) * 48 + yo, 8, stride=6), :] for xi in range(2)]
            dt[yo, xo] = jnp.concatenate(t, axis=0).astype(BF)


def lift(dt, s_ref, wl_ref, db, fp, pairs, count, index):
    for one, two in pairs:
        if two == one + 1:
            table = s_ref[:, 128 * one:128 * one + 256]
        else:
            table = jnp.concatenate([s_ref[:, 128 * one:128 * one + 128], s_ref[:, 128 * two:128 * two + 128]], axis=1)
        r = dot(rows([dt[b:b + 6] for b in range(3)]), table)
        r = r.astype(BF).reshape(6, 12, 16, 256)
        db[one] = r[..., :128]
        db[two] = r[..., 128:]
    first_slots = lax.broadcasted_iota(jnp.int32, (16, 128), 1) < 54

    def step(i, carry):
        q = index(i)
        for g in range(2):
            y = slice(3 * g, 3 * g + 3)
            ta = jnp.where(first_slots, db[q, y, 0:10], db[q, y, 1:11])
            r = act(dot(rows([ta, db[q, y, 2:12]]), wl_ref[...]))
            for half in range(2):
                part = r[:, 128 * half:128 * half + 128].reshape(3, 10, 16, 128)
                fp[2 * q + half, y] = part.astype(BF)
                if g == 0:
                    low_rows = part[0:2].reshape(40, 8, 128)
                    fp[2 * q + half, 6:8] = up_one(low_rows).reshape(2, 10, 16, 128).astype(BF)
        return carry

    lax.fori_loop(0, count, step, 0)


def encode(fp, fe, we_ref, sk, sd, base, count, index):
    low = lax.broadcasted_iota(jnp.int32, (16, 128), 1) < 64

    def edge_step(i, carry):
        q = index(i)
        fe[q] = jnp.where(low, fp[2 * q + 3], fp[2 * q])
        return carry

    lax.fori_loop(0, count, edge_step, 0)

    def step(i, carry):
        q = index(i)
        for g in range(2):
            y0 = 3 * g
            acc = None
            for lo, hi in ((0, 2), (2, 4), (4, 6), (6, 9)):
                parts = []
                for t in range(lo, hi):
                    a, b = t // 3, t % 3
                    sl = (slice(y0 + b, y0 + b + 3), slice(a, a + 8))
                    parts += [fp[(2 * q + 1,) + sl], fp[(2 * q + 2,) + sl], fe[(q,) + sl]]
                p = dot(rows(parts), we_ref[384 * lo:384 * hi, :])
                acc = p if acc is None else acc + p
            r = act(acc).reshape(3, 8, 2, 8, 256)
            for half in range(2):
                part = r[..., 128 * half:128 * half + 128]
                packed = part.reshape(3, 8, 16, 128).astype(BF)
                sp = 2 * q + half - base
                for yy in range(3):
                    yo = y0 + yy
                    sk[sp, yo // 2, yo % 2] = packed[yy].reshape(4, 2, 16, 128)
                    mixed = [jnp.concatenate([part[yy, (5 + xo) % 8, (5 + xo) // 8], part[yy, (7 + xo) % 8, (7 + xo) // 8]], axis=0)
                             for xo in range(4)]
                    mixed = jnp.stack(mixed).reshape(8, 8, 128)
                    if yo == 5:
                        sd[sp, 0] = mixed.reshape(4, 16, 128).astype(BF)
                    moved = up_one(mixed)
                    sd[sp, yo + 1] = moved.reshape(4, 16, 128).astype(BF)
                    if yo == 0:
                        sd[sp, 7] = up_one(moved).reshape(4, 16, 128).astype(BF)
        return carry

    lax.fori_loop(0, count, step, 0)


def inner_kernel(b0, b1, b2, b3, b4, s_ref, wl_ref, we_hbm, sk, sd, df, dt, db, fp, fe, we_ref, sem):
    copy = pltpu.make_async_copy(we_hbm, we_ref, sem)
    copy.start()
    for k, ref in enumerate((b0, b1, b2, b3, b4)):
        for x in range(4):
            df[192 * k + 48 * x:192 * k + 48 * x + 48] = ref[x].astype(F32)
    df[960:968] = jnp.zeros((8, 128), F32)
    tiles(df, dt)
    lift(dt, s_ref, wl_ref, db, fp, ((2, 3), (4, 5)), 4, lambda i: i + 2)
    copy.wait()
    encode(fp, fe, we_ref, sk, sd, 4, 3, lambda i: i + 2)


def outer_kernel(b0, b1, b2, b3, b4, left_ref, right_ref, x_ref, s_ref, wl_ref,
                 we_hbm, wd_hbm, w1_hbm, w2_hbm, wu_hbm, wj_hbm, wh_hbm, sk_hbm, sd_hbm, o_ref,
                 df, dt, db, fp, fe, sk, sd, c1, c2, de, uu, es, eu, hs,
                 we_ref, wd_ref, w1_ref, w2_ref, wu_ref, wj_ref, wh_ref, sems):
    plan = ((we_hbm, we_ref), (sk_hbm, sk.at[4:10]), (wd_hbm, wd_ref), (w1_hbm, w1_ref), (w2_hbm, w2_ref),
            (wu_hbm, wu_ref), (sd_hbm, sd.at[4:10]), (wj_hbm, wj_ref), (wh_hbm, wh_ref))
    copies = [pltpu.make_async_copy(src, dst, sems.at[i]) for i, (src, dst) in enumerate(plan)]
    for copy in copies:
        copy.start()

    lane = lax.broadcasted_iota(jnp.int32, (16, 128), 1)
    low = lane < 64
    for x in range(20):
        own = (b0, b1, b2, b3, b4)[x // 4][x % 4].astype(F32)
        left, right = left_ref[x].astype(F32), right_ref[x].astype(F32)
        for g in range(3):
            t = jnp.where(lane < 72, pltpu.roll(left, 48 - 24 * g if g < 2 else 0, 1) if g < 2 else left,
                          pltpu.roll(right, 72 - 24 * g, 1))
            df[48 * x + 16 * g:48 * x + 16 * g + 16] = jnp.where(lane < 48, own[16 * g:16 * g + 16], t)
    df[960:968] = jnp.zeros((8, 128), F32)
    tiles(df, dt)
    lift(dt, s_ref, wl_ref, db, fp, ((0, 1), (2, 5), (6, 7)), 6, lambda i: i + 2 * (i // 3))
    copies[0].wait()
    encode(fp, fe, we_ref, sk, sd, 0, 4, lambda i: i + 3 * (i // 2))

    copies[1].wait()
    copies[2].wait()
    r = act(dot(rows([sk[:, :, b, :, a] for a in range(2) for b in range(2)]), wd_ref[...]))
    r = r.reshape(7, 2, 3, 4, 2, 8, 128)
    for yo in range(3):
        for xo in range(5):
            t = jnp.stack([r[:, :, yo, xo % 4, xo // 4], r[:, :, yo, (3 + xo) % 4, (3 + xo) // 4]], axis=2)
            c1[:, :, yo, xo] = t.reshape(7, 2, 16, 128).astype(BF)
            if yo < 2:
                c1[:, :, yo + 3, xo] = up_one(t.reshape(28, 8, 128)).reshape(7, 2, 16, 128).astype(BF)

    def middle(src, w_ref, zp, xn):
        acc = None
        for t in range(9):
            a, b = t // 3, t % 3
            parts = [src[zi // 2:zi // 2 + zp, zi % 2, b:b + 3, a:a + xn] for zi in range(4)]
            p = dot(rows(parts), w_ref[512 * t:512 * t + 512, :])
            acc = p if acc is None else acc + p
        return act(acc).reshape(zp, 3, xn, 2, 8, 256)

    copies[3].wait()
    r = middle(c1, w1_ref, 6, 3)
    for half in range(2):
        part = r[..., 128 * half:128 * half + 128]
        for yo in range(3):
            for xo in range(4):
                t = jnp.stack([part[:, yo, xo % 3, xo // 3], part[:, yo, (2 + xo) % 3, (2 + xo) // 3]], axis=1)
                c2[:, half, yo, xo] = t.reshape(6, 16, 128).astype(BF)
                if yo < 2:
                    c2[:, half, yo + 3, xo] = up_one(t.reshape(12, 8, 128)).reshape(6, 16, 128).astype(BF)

    copies[4].wait()
    r = middle(c2, w2_ref, 5, 2).reshape(5, 3, 2, 16, 256).astype(BF)
    de[:, 0] = r[..., :128]
    de[:, 1] = r[..., 128:]

    copies[5].wait()
    r = act(dot(rows([de[...]]), wu_ref[...])).reshape(5, 2, 3, 2, 2, 8, 512)
    for yo in range(6):
        b = yo % 2
        for xo in range(4):
            t = []
            for f in (1 + xo, 3 + xo):
                a = f % 2
                n = 128 * (2 * a + b)
                t.append(r[:, :, yo // 2, (f // 2) % 2, f // 4, :, n:n + 128])
            t = jnp.stack(t, axis=2)
            if yo > 0:
                uu[:, :, yo - 1, xo] = t.reshape(5, 2, 16, 128).astype(BF)
            if yo < 3:
                uu[:, :, yo + 5, xo] = up_one(t.reshape(20, 8, 128)).reshape(5, 2, 16, 128).astype(BF)

    for k in (6, 7, 8):
        copies[k].wait()
    for q in range(4):
        es[q] = jnp.where(low, sd[2 * q + 5], sd[2 * q + 2])
        eu[q] = jnp.where(low, uu[q + 1, 1], uu[q, 0])

    for g in range(1):
        acc = None
        for t in range(9):
            a, b = t // 3, t % 3
            ys, xs = slice(b, b + 6), slice(a, a + 2)
            own = [jnp.stack([sd[2 * q + 3 + k, ys, xs] for q in range(4)]) for k in range(2)]
            parts = own + [es[:, ys, xs], uu[0:4, 1, ys, xs], uu[1:5, 0, ys, xs], eu[:, ys, xs]]
            p = dot(rows(parts), wj_ref[768 * t:768 * t + 768, :])
            acc = p if acc is None else acc + p
        j = act(acc).astype(BF).reshape(4, 192, 256)
        h = dot(jnp.concatenate([j[q] for q in range(4)], axis=1), wh_ref[...]).reshape(6, 2, 2, 8, 128)
        for yo in range(6):
            for x in range(4):
                hs[pl.ds(48 * x + yo, 8, stride=6), :] = h[yo, x % 2, x // 2]
    for x in range(4):
        t = jnp.transpose(hs[48 * x:48 * x + 32, :])
        for k in range(3):
            o_ref[k, x] = t[16 * k:16 * k + 16] + x_ref[k, x].astype(F32)


VM = pl.BlockSpec(memory_space=pltpu.VMEM)
ANY = pl.BlockSpec(memory_space=pl.ANY)


def call(body, args, specs, shapes, scratch=(), limit=16, flops=1_000_000):
    many = isinstance(shapes, list)
    return pl.pallas_call(
        body,
        out_shape=[jax.ShapeDtypeStruct(*x) for x in shapes] if many else jax.ShapeDtypeStruct(*shapes),
        in_specs=specs,
        out_specs=[VM] * len(shapes) if many else VM,
        scratch_shapes=scratch,
        compiler_params=pltpu.CompilerParams(vmem_limit_bytes=limit << 20),
        cost_estimate=pl.CostEstimate(flops=flops, bytes_accessed=2_000_000, transcendentals=0),
    )(*args)


def planes(d):
    return call(plane_kernel, (d,), [VM], [((4, 32, 128), BF), ((4, 8, 128), BF), ((4, 8, 128), BF)])


def rims(blocks):
    return call(rim_kernel, blocks, [VM] * 5, [((20, 16, 128), BF)] * 2)


V = pltpu.VMEM
FIELDS = [V((968, 128), F32), V((8, 12, 16, 128), BF), V((8, 6, 12, 16, 128), BF), V((16, 8, 10, 16, 128), BF), V((7, 8, 10, 16, 128), BF)]
PICK = picker()


def inner(blocks, ws):
    args = (*blocks, jnp.asarray(PICK, BF), ws[0], ws[1])
    return call(
        inner_kernel, args, [VM] * 7 + [ANY], [((6, 3, 2, 4, 2, 16, 128), BF), ((6, 8, 4, 16, 128), BF)],
        FIELDS + [V((3456, 256), BF), pltpu.SemaphoreType.DMA], limit=24, flops=8_000_000_000,
    )


def outer(blocks, left, right, d, ws, sk, sd):
    args = (*blocks, left, right, d, jnp.asarray(PICK, BF), *ws, sk, sd)
    return call(
        outer_kernel, args, [VM] * 10 + [ANY] * 9, ((3, 4, 16, 32), F32),
        FIELDS + [
            V((14, 3, 2, 4, 2, 16, 128), BF), V((14, 8, 4, 16, 128), BF), V((7, 2, 5, 5, 16, 128), BF),
            V((6, 2, 5, 4, 16, 128), BF), V((5, 2, 3, 2, 16, 128), BF), V((5, 2, 8, 4, 16, 128), BF),
            V((4, 8, 4, 16, 128), BF), V((4, 8, 4, 16, 128), BF), V((192, 128), F32),
            V((3456, 256), BF), V((512, 128), BF), V((4608, 256), BF), V((4608, 256), BF), V((128, 512), BF), V((6912, 256), BF),
            V((1024, 128), BF), pltpu.SemaphoreType.DMA((9,)),
        ], limit=44, flops=16_000_000_000,
    )


def local(displacement, *raw):
    d = jnp.swapaxes(displacement, 2, 3)
    own, top, bottom = planes(d)
    before, after = shift(top, "gy", 1), shift(bottom, "gy", -1)
    ws = weights(*raw)
    block = call(join_kernel, (before, own, after), [VM] * 3, ((4, 48, 128), BF))
    blocks = (shift(block, "gx", 2), shift(block, "gx", 1), block, shift(block, "gx", -1), shift(block, "gx", -2))
    left, right = rims(blocks)
    left, right = shift(left, "gz", 1), shift(right, "gz", -1)
    sk, sd = inner(blocks, ws)
    return jnp.swapaxes(outer(blocks, left, right, d, ws, sk, sd), 2, 3)


def solution(mesh):
    placed = (P(None, "gx", "gy", "gz"), P(), P(), P(), P(), P(), P(), P(), P())
    return jax.shard_map(local, mesh=mesh, in_specs=placed, out_specs=P(None, "gx", "gy", "gz"), check_vma=False)
```

```python
import jax
import jax.numpy as jnp
import numpy as np
from jax import lax
from jax.experimental import pallas as pl
from jax.experimental.pallas import tpu as pltpu
from jax.sharding import PartitionSpec as P

BF, F32 = jnp.bfloat16, jnp.float32
ENC = ((0, 2), (2, 4), (4, 6), (6, 9))


def shift(block, axis, step):
    count = lax.axis_size(axis)
    return lax.ppermute(block, axis, [(i, (i + step) % count) for i in range(count)])


def act(value):
    return jnp.maximum(value, 0.1 * value)


def pick(quads):
    row = lax.broadcasted_iota(jnp.int32, (128, 128), 0)
    lane = lax.broadcasted_iota(jnp.int32, (128, 128), 1)
    slot, ch, zi = lane // 18, lane % 18 // 6, lane % 6
    columns = []
    for q in quads:
        z = 4 * q - 1 + zi
        start = jnp.where(z < 8, 48, jnp.where(z < 16, 16, jnp.where(z < 24, -16, 48)))
        hit = (row == start + 8 * ch + z) & (slot < 6) & (z >= 0) & (z < 32)
        columns.append(jnp.concatenate([jnp.where(hit & (slot % 3 == b), 1.0, 0.0).astype(BF) for b in range(3)], axis=0))
    return jnp.concatenate(columns, axis=1)


def lift_picker():
    table = np.zeros((2, 256, 2, 128), np.float32)
    for t in range(9):
        for ch in range(3):
            for zi in range(6):
                for zo in range(4):
                    if 0 <= zi - zo < 3:
                        r = 18 * t + 6 * ch + zi if t < 6 else 128 + 18 * (t - 6) + 6 * ch + zi
                        table[zo // 2, r, zo % 2, 32 * ch + 3 * t + zi - zo] = 1
    return table.reshape(2, 256, 256)


def banded_kernel(l_ref, h_ref, p_ref, e_hbm, m1_hbm, m2_hbm, u_hbm, j_hbm, wb, w1, w2, wu, wj, wh,
                  e_ref, m1_ref, m2_ref, u_ref, j_ref, sems):
    plan = ((e_hbm, e_ref), (j_hbm, j_ref), (m1_hbm, m1_ref), (m2_hbm, m2_ref), (u_hbm, u_ref))
    copies = [pltpu.make_async_copy(src, dst, sems.at[i]) for i, (src, dst) in enumerate(plan)]
    for copy in copies:
        copy.start()

    table = jnp.concatenate([jnp.concatenate([l_ref[k].astype(F32), jnp.zeros((5, 64), F32)], axis=0) for k in range(3)], axis=0)
    table = jnp.concatenate([table, jnp.zeros((32, 64), F32)], axis=0)
    zero = jnp.zeros_like(table)
    table = jnp.concatenate([jnp.concatenate([table, zero], axis=1), jnp.concatenate([zero, table], axis=1)], axis=0).astype(BF)
    for p in range(2):
        wb[2304 + 256 * p:2560 + 256 * p] = dot(p_ref[p], table).astype(BF)

    column = jnp.transpose(jnp.concatenate([h_ref[...].astype(F32), jnp.zeros((5, 64), F32)], axis=0))
    lane = lax.broadcasted_iota(jnp.int32, (64, 128), 1)
    spread = jnp.zeros((64, 128), F32)
    for k in range(3):
        spread = jnp.where(lane // 16 == k, column[:, k:k + 1], spread)
    for z in range(16):
        wh[64 * z:64 * z + 64] = jnp.where(lane % 16 == z, spread, 0.0).astype(BF)

    def turned(value):
        return jnp.transpose(value.astype(F32)).astype(BF)

    def step(t, carry):
        for raw in (e_ref, j_ref):
            c = [raw[3 * t + k] for k in range(3)]
            o = jnp.zeros_like(c[0])
            for k, pair in enumerate(((c[0], o), (c[1], c[0]), (c[2], c[1]), (o, c[2]))):
                block = turned(jnp.concatenate(pair, axis=0))
                if raw is e_ref:
                    wb[pl.ds(pl.multiple_of(256 * t + 64 * k, 64), 64), :] = block
                else:
                    wj[t, k] = block
        for raw, out in ((m1_ref, w1), (m2_ref, w2)):
            for k in range(3):
                out[t, k] = turned(raw[3 * t + k])
        return carry

    for copy in copies[:4]:
        copy.wait()
    lax.fori_loop(0, 9, step, 0)
    copies[4].wait()
    for k in range(4):
        wu[:, 128 * k:128 * k + 128] = turned(jnp.concatenate([u_ref[2 * k], u_ref[2 * k + 1]], axis=0))


def weights(lift, encode, down, m1, m2, up, decode, head):
    shapes = ((2816, 128), (9, 3, 128, 128), (9, 3, 128, 128), (128, 512), (9, 4, 128, 128), (1024, 128))
    raw = (encode, m1, m2, up, decode)
    wb, w1, w2, wu, wj, wh = call(
        banded_kernel, (jnp.transpose(lift, (2, 0, 1)), head, jnp.asarray(LIFT_PICK, BF), *raw),
        [VM] * 3 + [HBM] * 5, [(shape, BF) for shape in shapes],
        [V(w.shape, BF) for w in raw] + [pltpu.SemaphoreType.DMA((5,))], limit=PREP, flops=6_000_000_000,
    )
    return wb, jnp.swapaxes(down, 1, 2).reshape(512, 128), w1, w2, wu, wj, wh


def quad_rows(blocks):
    o = jnp.zeros_like(blocks[0])
    columns = [[blocks[z - 2 * p + 1] if 0 <= z - 2 * p + 1 < 4 else o for z in (0, 1, 2, 3, 4, -1)] for p in range(2)]
    return jnp.concatenate([jnp.concatenate(c, axis=0) for c in columns], axis=1)


def pair_rows(blocks):
    o = jnp.zeros_like(blocks[0])
    columns = [[blocks[z - p] if 0 <= z - p < 3 else o for z in range(4)] for p in range(2)]
    return jnp.concatenate([jnp.concatenate(c, axis=0) for c in columns], axis=1)


def dot(a, b):
    return jnp.dot(a, b, preferred_element_type=F32)


def rows(parts):
    flat = [p.reshape(-1, p.shape[-1]) for p in parts]
    return flat[0] if len(flat) == 1 else jnp.concatenate(flat, axis=1)


def up_one(v):
    return pltpu.roll(v, v.shape[-2] - 1, v.ndim - 2)


def plane_kernel(d_ref, a_ref, top_ref, low_ref):
    for x in range(4):
        parts = [d_ref[k, x].astype(F32)[h:h + 8] for h in (8, 0) for k in range(3)]
        t = jnp.transpose(jnp.concatenate(parts, axis=0))
        t = jnp.concatenate([t, jnp.zeros((32, 80), F32)], axis=1)
        a_ref[x] = t.astype(BF)
        top_ref[x] = t[24:].astype(BF)
        low_ref[x] = t[:8].astype(BF)


def join_kernel(before_ref, a_ref, after_ref, o_ref):
    for x in range(4):
        parts = [r[x].astype(F32) for r in (before_ref, a_ref, after_ref)]
        o_ref[x] = jnp.concatenate(parts, axis=0).astype(BF)


def rim_kernel(b0, b1, b2, b3, b4, left_ref, right_ref):
    lane = lax.broadcasted_iota(jnp.int32, (16, 128), 1)
    for x in range(20):
        own = (b0, b1, b2, b3, b4)[x // 4][x % 4].astype(F32)
        for out, first in ((left_ref, 0), (right_ref, 24)):
            g = [own[16 * k:16 * k + 16] for k in range(3)]
            g = [t if 24 * k == first else pltpu.roll(t, (24 * k - first) % 128, 1) for k, t in enumerate(g)]
            out[x] = jnp.where(lane < 24, g[0], jnp.where(lane < 48, g[1], g[2])).astype(BF)


def tiles(df, dt):
    for yo in range(8):
        for xo in range(12):
            t = [df[pl.ds((8 * xi + xo) * 48 + yo, 8, stride=6), :] for xi in range(2)]
            dt[yo, xo] = jnp.concatenate(t, axis=0).astype(BF)


def lift(dt, wb_ref, db, fp, pairs, count, index):
    for one, two in pairs:
        table = pick((one, two))
        r = dot(rows([dt[b:b + 6] for b in range(3)]), table)
        r = r.astype(BF).reshape(6, 12, 16, 256)
        db[one] = r[..., :128]
        db[two] = r[..., 128:]
    first_slots = lax.broadcasted_iota(jnp.int32, (16, 128), 1) < 54

    def step(i, carry):
        q = index(i)
        for g in range(2):
            y = slice(3 * g, 3 * g + 3)
            ta = jnp.where(first_slots, db[q, y, 0:10], db[q, y, 1:11])
            table = jnp.concatenate([wb_ref[2304:2560], wb_ref[2560:2816]], axis=1)
            r = act(dot(rows([ta, db[q, y, 2:12]]), table))
            for half in range(2):
                part = r[:, 128 * half:128 * half + 128].reshape(3, 10, 16, 128)
                fp[2 * q + half, y] = part.astype(BF)
                if g == 0:
                    low_rows = part[0:2].reshape(40, 8, 128)
                    fp[2 * q + half, 6:8] = up_one(low_rows).reshape(2, 10, 16, 128).astype(BF)
        return carry

    lax.fori_loop(0, count, step, 0)


def encode(fp, fe, wb_ref, sk, sd, base, count, index):
    low = lax.broadcasted_iota(jnp.int32, (16, 128), 1) < 64

    def edge_step(i, carry):
        q = index(i)
        fe[q] = jnp.where(low, fp[2 * q + 3], fp[2 * q])
        return carry

    lax.fori_loop(0, count, edge_step, 0)

    def step(i, carry):
        q = index(i)
        for g in range(2):
            y0 = 3 * g
            acc = None
            for lo, hi in ENC:
                parts = []
                for t in range(lo, hi):
                    a, b = t // 3, t % 3
                    sl = (slice(y0 + b, y0 + b + 3), slice(a, a + 8))
                    parts += [fp[(2 * q + 1,) + sl], fp[(2 * q + 2,) + sl], fe[(q,) + sl]]
                p = dot(rows(parts), jnp.concatenate([quad_rows([wb_ref[256 * t + 64 * k:256 * t + 64 * k + 64] for k in range(4)]) for t in range(lo, hi)], axis=0))
                acc = p if acc is None else acc + p
            r = act(acc).reshape(3, 8, 2, 8, 256)
            for half in range(2):
                part = r[..., 128 * half:128 * half + 128]
                packed = part.reshape(3, 8, 16, 128).astype(BF)
                sp = 2 * q + half - base
                for yy in range(3):
                    yo = y0 + yy
                    sk[sp, yo // 2, yo % 2] = packed[yy].reshape(4, 2, 16, 128)
                    mixed = [jnp.concatenate([part[yy, (5 + xo) % 8, (5 + xo) // 8], part[yy, (7 + xo) % 8, (7 + xo) // 8]], axis=0)
                             for xo in range(4)]
                    mixed = jnp.stack(mixed).reshape(8, 8, 128)
                    if yo == 5:
                        sd[sp, 0] = mixed.reshape(4, 16, 128).astype(BF)
                    moved = up_one(mixed)
                    sd[sp, yo + 1] = moved.reshape(4, 16, 128).astype(BF)
                    if yo == 0:
                        sd[sp, 7] = up_one(moved).reshape(4, 16, 128).astype(BF)
        return carry

    lax.fori_loop(0, count, step, 0)


def inner_kernel(b0, b1, b2, b3, b4, wb_ref, sk, sd, df, dt, db, fp, fe):
    for k, ref in enumerate((b0, b1, b2, b3, b4)):
        for x in range(4):
            df[192 * k + 48 * x:192 * k + 48 * x + 48] = ref[x].astype(F32)
    df[960:968] = jnp.zeros((8, 128), F32)
    tiles(df, dt)
    lift(dt, wb_ref, db, fp, ((2, 3), (4, 5)), 4, lambda i: i + 2)
    encode(fp, fe, wb_ref, sk, sd, 4, 3, lambda i: i + 2)


def outer_kernel(b0, b1, b2, b3, b4, left_ref, right_ref, x_ref, wb_ref,
                 wd_ref, w1_ref, w2_ref, wu_ref, wj_ref, wh_ref, sk_in, sd_in, o_ref,
                 df, dt, db, fp, fe, sk, sd, c1, c2, de, uu, es, eu, hs, ac, sems):
    plan = ((sk_in, sk.at[4:10]), (sd_in, sd.at[4:10]))
    copies = [pltpu.make_async_copy(src, dst, sems.at[i]) for i, (src, dst) in enumerate(plan)]
    for copy in copies:
        copy.start()

    lane = lax.broadcasted_iota(jnp.int32, (16, 128), 1)
    low = lane < 64
    for x in range(20):
        own = (b0, b1, b2, b3, b4)[x // 4][x % 4].astype(F32)
        left, right = left_ref[x].astype(F32), right_ref[x].astype(F32)
        for g in range(3):
            t = jnp.where(lane < 72, pltpu.roll(left, 48 - 24 * g if g < 2 else 0, 1) if g < 2 else left,
                          pltpu.roll(right, 72 - 24 * g, 1))
            df[48 * x + 16 * g:48 * x + 16 * g + 16] = jnp.where(lane < 48, own[16 * g:16 * g + 16], t)
    df[960:968] = jnp.zeros((8, 128), F32)
    tiles(df, dt)
    lift(dt, wb_ref, db, fp, ((0, 1), (2, 5), (6, 7)), 6, lambda i: i + 2 * (i // 3))
    encode(fp, fe, wb_ref, sk, sd, 0, 4, lambda i: i + 3 * (i // 2))

    for copy in copies:
        copy.wait()
    r = act(dot(rows([sk[:, :, b, :, a] for a in range(2) for b in range(2)]), wd_ref[...]))
    r = r.reshape(7, 2, 3, 4, 2, 8, 128)
    for yo in range(3):
        for xo in range(5):
            t = jnp.stack([r[:, :, yo, xo % 4, xo // 4], r[:, :, yo, (3 + xo) % 4, (3 + xo) // 4]], axis=2)
            c1[:, :, yo, xo] = t.reshape(7, 2, 16, 128).astype(BF)
            if yo < 2:
                c1[:, :, yo + 3, xo] = up_one(t.reshape(28, 8, 128)).reshape(7, 2, 16, 128).astype(BF)

    def middle(src, w_ref, zp, xn):
        m = zp * xn * 48
        ac[:m] = jnp.zeros((m, 256), F32)

        def tap(a, carry):
            parts, table = [], []
            for b in range(3):
                parts += [src[zi // 2:zi // 2 + zp, zi % 2, b:b + 3, pl.ds(a, xn)] for zi in range(4)]
                table.append(pair_rows([w_ref[3 * a + b, k] for k in range(3)]))
            ac[:m] += dot(rows(parts), jnp.concatenate(table, axis=0))
            return carry

        lax.fori_loop(0, 3, tap, 0)
        return act(ac[:m]).reshape(zp, 3, xn, 2, 8, 256)

    r = middle(c1, w1_ref, 6, 3)
    for half in range(2):
        part = r[..., 128 * half:128 * half + 128]
        for yo in range(3):
            for xo in range(4):
                t = jnp.stack([part[:, yo, xo % 3, xo // 3], part[:, yo, (2 + xo) % 3, (2 + xo) // 3]], axis=1)
                c2[:, half, yo, xo] = t.reshape(6, 16, 128).astype(BF)
                if yo < 2:
                    c2[:, half, yo + 3, xo] = up_one(t.reshape(12, 8, 128)).reshape(6, 16, 128).astype(BF)

    r = middle(c2, w2_ref, 5, 2).reshape(5, 3, 2, 16, 256).astype(BF)
    de[:, 0] = r[..., :128]
    de[:, 1] = r[..., 128:]

    r = act(dot(rows([de[...]]), wu_ref[...])).reshape(5, 2, 3, 2, 2, 8, 512)
    for yo in range(6):
        b = yo % 2
        for xo in range(4):
            t = []
            for f in (1 + xo, 3 + xo):
                a = f % 2
                n = 128 * (2 * a + b)
                t.append(r[:, :, yo // 2, (f // 2) % 2, f // 4, :, n:n + 128])
            t = jnp.stack(t, axis=2)
            if yo > 0:
                uu[:, :, yo - 1, xo] = t.reshape(5, 2, 16, 128).astype(BF)
            if yo < 3:
                uu[:, :, yo + 5, xo] = up_one(t.reshape(20, 8, 128)).reshape(5, 2, 16, 128).astype(BF)

    for q in range(4):
        es[q] = jnp.where(low, sd[2 * q + 5], sd[2 * q + 2])
        eu[q] = jnp.where(low, uu[q + 1, 1], uu[q, 0])

    if True:
        ac[:768] = jnp.zeros((768, 256), F32)

        def tap(a, carry):
            parts, table = [], []
            for b in range(3):
                ys, xs, t = slice(b, b + 6), pl.ds(a, 2), 3 * a + b
                own = [jnp.stack([sd[2 * q + 3 + k, ys, xs] for q in range(4)]) for k in range(2)]
                parts += own + [es[:, ys, xs], uu[0:4, 1, ys, xs], uu[1:5, 0, ys, xs], eu[:, ys, xs]]
                blocks = [wj_ref[t, k] for k in range(4)]
                table += [quad_rows([w[:64] for w in blocks]), quad_rows([w[64:] for w in blocks])]
            ac[:768] += dot(rows(parts), jnp.concatenate(table, axis=0))
            return carry

        lax.fori_loop(0, 3, tap, 0)
        acc = ac[:768]
        j = act(acc).astype(BF).reshape(4, 192, 256)
        h = dot(jnp.concatenate([j[q] for q in range(4)], axis=1), wh_ref[...]).reshape(6, 2, 2, 8, 128)
        for yo in range(6):
            for x in range(4):
                hs[pl.ds(48 * x + yo, 8, stride=6), :] = h[yo, x % 2, x // 2]
    for x in range(4):
        t = jnp.transpose(hs[48 * x:48 * x + 32, :])
        for k in range(3):
            o_ref[k, x] = t[16 * k:16 * k + 16] + x_ref[k, x].astype(F32)


VM = pl.BlockSpec(memory_space=pltpu.VMEM)
HBM = pl.BlockSpec(memory_space=pltpu.HBM)


def call(body, args, specs, shapes, scratch=(), limit=16, flops=1_000_000):
    many = isinstance(shapes, list)
    return pl.pallas_call(
        body,
        out_shape=[jax.ShapeDtypeStruct(*x) for x in shapes] if many else jax.ShapeDtypeStruct(*shapes),
        in_specs=specs,
        out_specs=[VM] * len(shapes) if many else VM,
        scratch_shapes=scratch,
        compiler_params=pltpu.CompilerParams(vmem_limit_bytes=limit << 20),
        cost_estimate=pl.CostEstimate(flops=flops, bytes_accessed=2_000_000, transcendentals=0),
    )(*args)


def planes(d):
    return call(plane_kernel, (d,), [VM], [((4, 32, 128), BF), ((4, 8, 128), BF), ((4, 8, 128), BF)])


def rims(blocks):
    return call(rim_kernel, blocks, [VM] * 5, [((20, 16, 128), BF)] * 2)


V = pltpu.VMEM
FIELDS = [V((968, 128), F32), V((8, 12, 16, 128), BF), V((8, 6, 12, 16, 128), BF), V((16, 8, 10, 16, 128), BF), V((7, 8, 10, 16, 128), BF)]
PREP, INNER, OUTER = 58, 20, 30
LIFT_PICK = lift_picker()


def inner(blocks, ws):
    args = (*blocks, ws[0])
    return call(
        inner_kernel, args, [VM] * 6, [((6, 3, 2, 4, 2, 16, 128), BF), ((6, 8, 4, 16, 128), BF)],
        FIELDS, limit=INNER, flops=8_000_000_000,
    )


def outer(blocks, left, right, d, ws, sk, sd):
    args = (*blocks, left, right, d, *ws, sk, sd)
    return call(
        outer_kernel, args, [VM] * 17, ((3, 4, 16, 32), F32),
        FIELDS + [
            V((14, 3, 2, 4, 2, 16, 128), BF), V((14, 8, 4, 16, 128), BF), V((7, 2, 5, 5, 16, 128), BF),
            V((6, 2, 5, 4, 16, 128), BF), V((5, 2, 3, 2, 16, 128), BF), V((5, 2, 8, 4, 16, 128), BF),
            V((4, 8, 4, 16, 128), BF), V((4, 8, 4, 16, 128), BF), V((192, 128), F32),
            V((864, 256), F32), pltpu.SemaphoreType.DMA((2,)),
        ], limit=OUTER, flops=16_000_000_000,
    )


def local(displacement, *raw):
    d = jnp.swapaxes(displacement, 2, 3)
    own, top, bottom = planes(d)
    before, after = shift(top, "gy", 1), shift(bottom, "gy", -1)
    ws = weights(*raw)
    block = call(join_kernel, (before, own, after), [VM] * 3, ((4, 48, 128), BF))
    blocks = (shift(block, "gx", 2), shift(block, "gx", 1), block, shift(block, "gx", -1), shift(block, "gx", -2))
    left, right = rims(blocks)
    left, right = shift(left, "gz", 1), shift(right, "gz", -1)
    sk, sd = inner(blocks, ws)
    return jnp.swapaxes(outer(blocks, left, right, d, ws, sk, sd), 2, 3)


def solution(mesh):
    placed = (P(None, "gx", "gy", "gz"), P(), P(), P(), P(), P(), P(), P(), P())
    return jax.shard_map(local, mesh=mesh, in_specs=placed, out_specs=P(None, "gx", "gy", "gz"), check_vma=False)
```

```python
import jax
import jax.numpy as jnp
import numpy as np
from jax import lax
from jax.experimental import pallas as pl
from jax.experimental.pallas import tpu as pltpu
from jax.sharding import PartitionSpec as P

BF, F32 = jnp.bfloat16, jnp.float32
ENC = ((0, 2), (2, 4), (4, 6), (6, 9))


def shift(block, axis, step):
    count = lax.axis_size(axis)
    return lax.ppermute(block, axis, [(i, (i + step) % count) for i in range(count)])


def act(value):
    return jnp.maximum(value, 0.1 * value)


def pick(quads):
    row = lax.broadcasted_iota(jnp.int32, (128, 128), 0)
    lane = lax.broadcasted_iota(jnp.int32, (128, 128), 1)
    slot, ch, zi = lane // 18, lane % 18 // 6, lane % 6
    columns = []
    for q in quads:
        z = 4 * q - 1 + zi
        start = jnp.where(z < 8, 48, jnp.where(z < 16, 16, jnp.where(z < 24, -16, 48)))
        hit = (row == start + 8 * ch + z) & (slot < 6) & (z >= 0) & (z < 32)
        columns.append(jnp.concatenate([jnp.where(hit & (slot % 3 == b), 1.0, 0.0).astype(BF) for b in range(3)], axis=0))
    return jnp.concatenate(columns, axis=1)


def lift_picker():
    table = np.zeros((2, 256, 2, 128), np.float32)
    for t in range(9):
        for ch in range(3):
            for zi in range(6):
                for zo in range(4):
                    if 0 <= zi - zo < 3:
                        r = 18 * t + 6 * ch + zi if t < 6 else 128 + 18 * (t - 6) + 6 * ch + zi
                        table[zo // 2, r, zo % 2, 32 * ch + 3 * t + zi - zo] = 1
    return table.reshape(2, 256, 256)


def banded_kernel(l_ref, h_ref, p_ref, e_hbm, m1_hbm, m2_hbm, u_hbm, j_hbm, wb, w1, w2, wu, wj, wh,
                  e_ref, m1_ref, m2_ref, u_ref, j_ref, sems):
    plan = ((e_hbm, e_ref), (j_hbm, j_ref), (m1_hbm, m1_ref), (m2_hbm, m2_ref), (u_hbm, u_ref))
    copies = [pltpu.make_async_copy(src, dst, sems.at[i]) for i, (src, dst) in enumerate(plan)]
    for copy in copies:
        copy.start()

    table = jnp.concatenate([jnp.concatenate([l_ref[k].astype(F32), jnp.zeros((5, 64), F32)], axis=0) for k in range(3)], axis=0)
    table = jnp.concatenate([table, jnp.zeros((32, 64), F32)], axis=0)
    zero = jnp.zeros_like(table)
    table = jnp.concatenate([jnp.concatenate([table, zero], axis=1), jnp.concatenate([zero, table], axis=1)], axis=0).astype(BF)
    for p in range(2):
        wb[2304 + 256 * p:2560 + 256 * p] = dot(p_ref[p], table).astype(BF)

    column = jnp.transpose(jnp.concatenate([h_ref[...].astype(F32), jnp.zeros((5, 64), F32)], axis=0))
    lane = lax.broadcasted_iota(jnp.int32, (64, 128), 1)
    spread = jnp.zeros((64, 128), F32)
    for k in range(3):
        spread = jnp.where(lane // 16 == k, column[:, k:k + 1], spread)
    for z in range(16):
        wh[64 * z:64 * z + 64] = jnp.where(lane % 16 == z, spread, 0.0).astype(BF)

    def turned(value):
        return jnp.transpose(value.astype(F32)).astype(BF)

    def step(t, carry):
        for raw in (e_ref, j_ref):
            c = [raw[3 * t + k] for k in range(3)]
            o = jnp.zeros_like(c[0])
            for k, pair in enumerate(((c[0], o), (c[1], c[0]), (c[2], c[1]), (o, c[2]))):
                block = turned(jnp.concatenate(pair, axis=0))
                if raw is e_ref:
                    wb[pl.ds(pl.multiple_of(256 * t + 64 * k, 64), 64), :] = block
                else:
                    wj[t, k] = block
        for raw, out in ((m1_ref, w1), (m2_ref, w2)):
            for k in range(3):
                out[t, k] = turned(raw[3 * t + k])
        return carry

    for copy in copies[:4]:
        copy.wait()
    lax.fori_loop(0, 9, step, 0)
    copies[4].wait()
    for k in range(4):
        wu[:, 128 * k:128 * k + 128] = turned(jnp.concatenate([u_ref[2 * k], u_ref[2 * k + 1]], axis=0))


def weights(lift, encode, down, m1, m2, up, decode, head):
    shapes = ((2816, 128), (9, 3, 128, 128), (9, 3, 128, 128), (128, 512), (9, 4, 128, 128), (1024, 128))
    raw = (encode, m1, m2, up, decode)
    wb, w1, w2, wu, wj, wh = call(
        banded_kernel, (jnp.transpose(lift, (2, 0, 1)), head, jnp.asarray(LIFT_PICK, BF), *raw),
        [VM] * 3 + [HBM] * 5, [(shape, BF) for shape in shapes],
        [V(w.shape, BF) for w in raw] + [pltpu.SemaphoreType.DMA((5,))], limit=PREP, flops=6_000_000_000,
    )
    return wb, jnp.swapaxes(down, 1, 2).reshape(512, 128), w1, w2, wu, wj, wh


def quad_rows(blocks):
    o = jnp.zeros_like(blocks[0])
    columns = [[blocks[z - 2 * p + 1] if 0 <= z - 2 * p + 1 < 4 else o for z in (0, 1, 2, 3, 4, -1)] for p in range(2)]
    return jnp.concatenate([jnp.concatenate(c, axis=0) for c in columns], axis=1)


def pair_rows(blocks):
    o = jnp.zeros_like(blocks[0])
    columns = [[blocks[z - p] if 0 <= z - p < 3 else o for z in range(4)] for p in range(2)]
    return jnp.concatenate([jnp.concatenate(c, axis=0) for c in columns], axis=1)


def dot(a, b):
    return jnp.dot(a, b, preferred_element_type=F32)


def rows(parts):
    flat = [p.reshape(-1, p.shape[-1]) for p in parts]
    return flat[0] if len(flat) == 1 else jnp.concatenate(flat, axis=1)


def up_one(v):
    return pltpu.roll(v, v.shape[-2] - 1, v.ndim - 2)


def plane_kernel(d_ref, a_ref, top_ref, low_ref):
    for x in range(4):
        parts = [d_ref[k, x].astype(F32)[h:h + 8] for h in (8, 0) for k in range(3)]
        t = jnp.transpose(jnp.concatenate(parts, axis=0))
        t = jnp.concatenate([t, jnp.zeros((32, 80), F32)], axis=1)
        a_ref[x] = t.astype(BF)
        top_ref[x] = t[24:].astype(BF)
        low_ref[x] = t[:8].astype(BF)


def join_kernel(before_ref, a_ref, after_ref, o_ref):
    for x in range(4):
        parts = [r[x].astype(F32) for r in (before_ref, a_ref, after_ref)]
        o_ref[x] = jnp.concatenate(parts, axis=0).astype(BF)


def rim_kernel(b0, b1, b2, b3, b4, left_ref, right_ref):
    lane = lax.broadcasted_iota(jnp.int32, (16, 128), 1)
    for x in range(20):
        own = (b0, b1, b2, b3, b4)[x // 4][x % 4].astype(F32)
        for out, first in ((left_ref, 0), (right_ref, 24)):
            g = [own[16 * k:16 * k + 16] for k in range(3)]
            g = [t if 24 * k == first else pltpu.roll(t, (24 * k - first) % 128, 1) for k, t in enumerate(g)]
            out[x] = jnp.where(lane < 24, g[0], jnp.where(lane < 48, g[1], g[2])).astype(BF)


def tiles(df, dt):
    for yo in range(8):
        for xo in range(12):
            t = [df[pl.ds((8 * xi + xo) * 48 + yo, 8, stride=6), :] for xi in range(2)]
            dt[yo, xo] = jnp.concatenate(t, axis=0).astype(BF)


def lift(dt, wb_ref, db, fp, pairs, count, index):
    for one, two in pairs:
        table = pick((one, two))
        r = dot(rows([dt[b:b + 6] for b in range(3)]), table)
        r = r.astype(BF).reshape(6, 12, 16, 256)
        db[one] = r[..., :128]
        db[two] = r[..., 128:]
    first_slots = lax.broadcasted_iota(jnp.int32, (16, 128), 1) < 54

    def step(i, carry):
        q = index(i)
        for g in range(2):
            y = slice(3 * g, 3 * g + 3)
            ta = jnp.where(first_slots, db[q, y, 0:10], db[q, y, 1:11])
            table = jnp.concatenate([wb_ref[2304:2560], wb_ref[2560:2816]], axis=1)
            r = act(dot(rows([ta, db[q, y, 2:12]]), table))
            for half in range(2):
                part = r[:, 128 * half:128 * half + 128].reshape(3, 10, 16, 128)
                fp[2 * q + half, y] = part.astype(BF)
                if g == 0:
                    low_rows = part[0:2].reshape(40, 8, 128)
                    fp[2 * q + half, 6:8] = up_one(low_rows).reshape(2, 10, 16, 128).astype(BF)
        return carry

    lax.fori_loop(0, count, step, 0)


def encode(fp, fe, wb_ref, sk, sd, base, count, index):
    low = lax.broadcasted_iota(jnp.int32, (16, 128), 1) < 64

    def edge_step(i, carry):
        q = index(i)
        fe[q] = jnp.where(low, fp[2 * q + 3], fp[2 * q])
        return carry

    lax.fori_loop(0, count, edge_step, 0)

    def step(i, carry):
        q = index(i)
        for g in range(2):
            y0 = 3 * g
            acc = None
            for lo, hi in ENC:
                parts = []
                for t in range(lo, hi):
                    a, b = t // 3, t % 3
                    sl = (slice(y0 + b, y0 + b + 3), slice(a, a + 8))
                    parts += [fp[(2 * q + 1,) + sl], fp[(2 * q + 2,) + sl], fe[(q,) + sl]]
                p = dot(rows(parts), jnp.concatenate([quad_rows([wb_ref[256 * t + 64 * k:256 * t + 64 * k + 64] for k in range(4)]) for t in range(lo, hi)], axis=0))
                acc = p if acc is None else acc + p
            r = act(acc).reshape(3, 8, 2, 8, 256)
            for half in range(2):
                part = r[..., 128 * half:128 * half + 128]
                packed = part.reshape(3, 8, 16, 128).astype(BF)
                sp = 2 * q + half - base
                for yy in range(3):
                    yo = y0 + yy
                    sk[sp, yo // 2, yo % 2] = packed[yy].reshape(4, 2, 16, 128)
                    mixed = [jnp.concatenate([part[yy, (5 + xo) % 8, (5 + xo) // 8], part[yy, (7 + xo) % 8, (7 + xo) // 8]], axis=0)
                             for xo in range(4)]
                    mixed = jnp.stack(mixed).reshape(8, 8, 128)
                    if yo == 5:
                        sd[sp, 0] = mixed.reshape(4, 16, 128).astype(BF)
                    moved = up_one(mixed)
                    sd[sp, yo + 1] = moved.reshape(4, 16, 128).astype(BF)
                    if yo == 0:
                        sd[sp, 7] = up_one(moved).reshape(4, 16, 128).astype(BF)
        return carry

    lax.fori_loop(0, count, step, 0)


def inner_kernel(b0, b1, b2, b3, b4, wb_ref, sk, sd, df, dt, db, fp, fe):
    for k, ref in enumerate((b0, b1, b2, b3, b4)):
        for x in range(4):
            df[192 * k + 48 * x:192 * k + 48 * x + 48] = ref[x].astype(F32)
    df[960:968] = jnp.zeros((8, 128), F32)
    tiles(df, dt)
    lift(dt, wb_ref, db, fp, ((2, 3), (4, 5)), 4, lambda i: i + 2)
    encode(fp, fe, wb_ref, sk, sd, 4, 3, lambda i: i + 2)


def outer_kernel(b0, b1, b2, b3, b4, left_ref, right_ref, x_ref, wb_ref,
                 wd_ref, w1_ref, w2_ref, wu_ref, wj_ref, wh_ref, sk_in, sd_in, o_ref,
                 df, dt, db, fp, fe, sk, sd, c1, c2, de, uu, es, eu, hs, ac, sems):
    plan = ((sk_in, sk.at[4:10]), (sd_in, sd.at[4:10]))
    copies = [pltpu.make_async_copy(src, dst, sems.at[i]) for i, (src, dst) in enumerate(plan)]
    for copy in copies:
        copy.start()

    lane = lax.broadcasted_iota(jnp.int32, (16, 128), 1)
    low = lane < 64
    for x in range(20):
        own = (b0, b1, b2, b3, b4)[x // 4][x % 4].astype(F32)
        left, right = left_ref[x].astype(F32), right_ref[x].astype(F32)
        for g in range(3):
            t = jnp.where(lane < 72, pltpu.roll(left, 48 - 24 * g if g < 2 else 0, 1) if g < 2 else left,
                          pltpu.roll(right, 72 - 24 * g, 1))
            df[48 * x + 16 * g:48 * x + 16 * g + 16] = jnp.where(lane < 48, own[16 * g:16 * g + 16], t)
    df[960:968] = jnp.zeros((8, 128), F32)
    tiles(df, dt)
    lift(dt, wb_ref, db, fp, ((0, 1), (2, 5), (6, 7)), 6, lambda i: i + 2 * (i // 3))
    encode(fp, fe, wb_ref, sk, sd, 0, 4, lambda i: i + 3 * (i // 2))

    for copy in copies:
        copy.wait()
    r = act(dot(rows([sk[:, :, b, :, a] for a in range(2) for b in range(2)]), wd_ref[...]))
    r = r.reshape(7, 2, 3, 4, 2, 8, 128)
    for yo in range(3):
        for xo in range(5):
            t = jnp.stack([r[:, :, yo, xo % 4, xo // 4], r[:, :, yo, (3 + xo) % 4, (3 + xo) // 4]], axis=2)
            c1[:, :, yo, xo] = t.reshape(7, 2, 16, 128).astype(BF)
            if yo < 2:
                c1[:, :, yo + 3, xo] = up_one(t.reshape(28, 8, 128)).reshape(7, 2, 16, 128).astype(BF)

    def middle(src, w_ref, zp, xn):
        m = zp * xn * 48
        ac[:m] = jnp.zeros((m, 256), F32)

        def tap(a, carry):
            parts, table = [], []
            for b in range(3):
                parts += [src[zi // 2:zi // 2 + zp, zi % 2, b:b + 3, pl.ds(a, xn)] for zi in range(4)]
                table.append(pair_rows([w_ref[3 * a + b, k] for k in range(3)]))
            ac[:m] += dot(rows(parts), jnp.concatenate(table, axis=0))
            return carry

        lax.fori_loop(0, 3, tap, 0)
        return act(ac[:m]).reshape(zp, 3, xn, 2, 8, 256)

    r = middle(c1, w1_ref, 6, 3)
    for half in range(2):
        part = r[..., 128 * half:128 * half + 128]
        for yo in range(3):
            for xo in range(4):
                t = jnp.stack([part[:, yo, xo % 3, xo // 3], part[:, yo, (2 + xo) % 3, (2 + xo) // 3]], axis=1)
                c2[:, half, yo, xo] = t.reshape(6, 16, 128).astype(BF)
                if yo < 2:
                    c2[:, half, yo + 3, xo] = up_one(t.reshape(12, 8, 128)).reshape(6, 16, 128).astype(BF)

    r = middle(c2, w2_ref, 5, 2).reshape(5, 3, 2, 16, 256).astype(BF)
    de[:, 0] = r[..., :128]
    de[:, 1] = r[..., 128:]

    r = act(dot(rows([de[...]]), wu_ref[...])).reshape(5, 2, 3, 2, 2, 8, 512)
    for yo in range(6):
        b = yo % 2
        for xo in range(4):
            t = []
            for f in (1 + xo, 3 + xo):
                a = f % 2
                n = 128 * (2 * a + b)
                t.append(r[:, :, yo // 2, (f // 2) % 2, f // 4, :, n:n + 128])
            t = jnp.stack(t, axis=2)
            if yo > 0:
                uu[:, :, yo - 1, xo] = t.reshape(5, 2, 16, 128).astype(BF)
            if yo < 3:
                uu[:, :, yo + 5, xo] = up_one(t.reshape(20, 8, 128)).reshape(5, 2, 16, 128).astype(BF)

    for q in range(4):
        es[q] = jnp.where(low, sd[2 * q + 5], sd[2 * q + 2])
        eu[q] = jnp.where(low, uu[q + 1, 1], uu[q, 0])

    if True:
        ac[:768] = jnp.zeros((768, 256), F32)

        def tap(a, carry):
            parts, table = [], []
            for b in range(3):
                ys, xs, t = slice(b, b + 6), pl.ds(a, 2), 3 * a + b
                own = [jnp.stack([sd[2 * q + 3 + k, ys, xs] for q in range(4)]) for k in range(2)]
                parts += own + [es[:, ys, xs], uu[0:4, 1, ys, xs], uu[1:5, 0, ys, xs], eu[:, ys, xs]]
                blocks = [wj_ref[t, k] for k in range(4)]
                table += [quad_rows([w[:64] for w in blocks]), quad_rows([w[64:] for w in blocks])]
            ac[:768] += dot(rows(parts), jnp.concatenate(table, axis=0))
            return carry

        lax.fori_loop(0, 3, tap, 0)
        acc = ac[:768]
        j = act(acc).astype(BF).reshape(4, 192, 256)
        h = dot(jnp.concatenate([j[q] for q in range(4)], axis=1), wh_ref[...]).reshape(6, 2, 2, 8, 128)
        for yo in range(6):
            for x in range(4):
                hs[pl.ds(48 * x + yo, 8, stride=6), :] = h[yo, x % 2, x // 2]
    for x in range(4):
        t = jnp.transpose(hs[48 * x:48 * x + 32, :])
        for k in range(3):
            o_ref[k, x] = t[16 * k:16 * k + 16] + x_ref[k, x].astype(F32)


VM = pl.BlockSpec(memory_space=pltpu.VMEM)
HBM = pl.BlockSpec(memory_space=pltpu.HBM)


def call(body, args, specs, shapes, scratch=(), limit=16, flops=1_000_000):
    many = isinstance(shapes, list)
    return pl.pallas_call(
        body,
        out_shape=[jax.ShapeDtypeStruct(*x) for x in shapes] if many else jax.ShapeDtypeStruct(*shapes),
        in_specs=specs,
        out_specs=[VM] * len(shapes) if many else VM,
        scratch_shapes=scratch,
        compiler_params=pltpu.CompilerParams(vmem_limit_bytes=limit << 20),
        cost_estimate=pl.CostEstimate(flops=flops, bytes_accessed=2_000_000, transcendentals=0),
    )(*args)


def planes(d):
    return call(plane_kernel, (d,), [VM], [((4, 32, 128), BF), ((4, 8, 128), BF), ((4, 8, 128), BF)])


def rims(blocks):
    return call(rim_kernel, blocks, [VM] * 5, [((20, 16, 128), BF)] * 2, flops=4_000_000_000)


V = pltpu.VMEM
FIELDS = [V((968, 128), F32), V((8, 12, 16, 128), BF), V((8, 6, 12, 16, 128), BF), V((16, 8, 10, 16, 128), BF), V((7, 8, 10, 16, 128), BF)]
PREP, INNER, OUTER = 58, 20, 30
LIFT_PICK = lift_picker()


def inner(blocks, ws):
    args = (*blocks, ws[0])
    return call(
        inner_kernel, args, [VM] * 6, [((6, 3, 2, 4, 2, 16, 128), BF), ((6, 8, 4, 16, 128), BF)],
        FIELDS, limit=INNER, flops=8_000_000_000,
    )


def outer(blocks, left, right, d, ws, sk, sd):
    args = (*blocks, left, right, d, *ws, sk, sd)
    return call(
        outer_kernel, args, [VM] * 17, ((3, 4, 16, 32), F32),
        FIELDS + [
            V((14, 3, 2, 4, 2, 16, 128), BF), V((14, 8, 4, 16, 128), BF), V((7, 2, 5, 5, 16, 128), BF),
            V((6, 2, 5, 4, 16, 128), BF), V((5, 2, 3, 2, 16, 128), BF), V((5, 2, 8, 4, 16, 128), BF),
            V((4, 8, 4, 16, 128), BF), V((4, 8, 4, 16, 128), BF), V((192, 128), F32),
            V((864, 256), F32), pltpu.SemaphoreType.DMA((2,)),
        ], limit=OUTER, flops=16_000_000_000,
    )


def local(displacement, *raw):
    d = jnp.swapaxes(displacement, 2, 3)
    own, top, bottom = planes(d)
    before, after = shift(top, "gy", 1), shift(bottom, "gy", -1)
    ws = weights(*raw)
    block = call(join_kernel, (before, own, after), [VM] * 3, ((4, 48, 128), BF))
    blocks = (shift(block, "gx", 2), shift(block, "gx", 1), block, shift(block, "gx", -1), shift(block, "gx", -2))
    left, right = rims(blocks)
    left, right = shift(left, "gz", 1), shift(right, "gz", -1)
    sk, sd = inner(blocks, ws)
    return jnp.swapaxes(outer(blocks, left, right, d, ws, sk, sd), 2, 3)


def solution(mesh):
    placed = (P(None, "gx", "gy", "gz"), P(), P(), P(), P(), P(), P(), P(), P())
    return jax.shard_map(local, mesh=mesh, in_specs=placed, out_specs=P(None, "gx", "gy", "gz"), check_vma=False)
```

```python
import jax
import jax.numpy as jnp
import numpy as np
from jax import lax
from jax.experimental import pallas as pl
from jax.experimental.pallas import tpu as pltpu
from jax.sharding import PartitionSpec as P

BF, F32 = jnp.bfloat16, jnp.float32
ENC = ((0, 2), (2, 4), (4, 6), (6, 9))


def shift(block, axis, step):
    count = lax.axis_size(axis)
    return lax.ppermute(block, axis, [(i, (i + step) % count) for i in range(count)])


def act(value):
    return jnp.maximum(value, 0.1 * value)


def pick(quads):
    row = lax.broadcasted_iota(jnp.int32, (128, 128), 0)
    lane = lax.broadcasted_iota(jnp.int32, (128, 128), 1)
    slot, ch, zi = lane // 18, lane % 18 // 6, lane % 6
    columns = []
    for q in quads:
        z = 4 * q - 1 + zi
        start = jnp.where(z < 8, 48, jnp.where(z < 16, 16, jnp.where(z < 24, -16, 48)))
        hit = (row == start + 8 * ch + z) & (slot < 6) & (z >= 0) & (z < 32)
        columns.append(jnp.concatenate([jnp.where(hit & (slot % 3 == b), 1.0, 0.0).astype(BF) for b in range(3)], axis=0))
    return jnp.concatenate(columns, axis=1)


def lift_picker():
    table = np.zeros((2, 256, 2, 128), np.float32)
    for t in range(9):
        for ch in range(3):
            for zi in range(6):
                for zo in range(4):
                    if 0 <= zi - zo < 3:
                        r = 18 * t + 6 * ch + zi if t < 6 else 128 + 18 * (t - 6) + 6 * ch + zi
                        table[zo // 2, r, zo % 2, 32 * ch + 3 * t + zi - zo] = 1
    return table.reshape(2, 256, 256)


def banded_kernel(l_ref, h_ref, p_ref, e_hbm, m1_hbm, m2_hbm, u_hbm, j_hbm, wb, w1, w2, wu, wj, wh,
                  e_ref, m1_ref, m2_ref, u_ref, j_ref, sems):
    plan = ((e_hbm, e_ref), (j_hbm, j_ref), (m1_hbm, m1_ref), (m2_hbm, m2_ref), (u_hbm, u_ref))
    copies = [pltpu.make_async_copy(src, dst, sems.at[i]) for i, (src, dst) in enumerate(plan)]
    for copy in copies:
        copy.start()

    table = jnp.concatenate([jnp.concatenate([l_ref[k].astype(F32), jnp.zeros((5, 64), F32)], axis=0) for k in range(3)], axis=0)
    table = jnp.concatenate([table, jnp.zeros((32, 64), F32)], axis=0)
    zero = jnp.zeros_like(table)
    table = jnp.concatenate([jnp.concatenate([table, zero], axis=1), jnp.concatenate([zero, table], axis=1)], axis=0).astype(BF)
    for p in range(2):
        wb[2304 + 256 * p:2560 + 256 * p] = dot(p_ref[p], table).astype(BF)

    column = jnp.transpose(jnp.concatenate([h_ref[...].astype(F32), jnp.zeros((5, 64), F32)], axis=0))
    lane = lax.broadcasted_iota(jnp.int32, (64, 128), 1)
    spread = jnp.zeros((64, 128), F32)
    for k in range(3):
        spread = jnp.where(lane // 16 == k, column[:, k:k + 1], spread)
    for z in range(16):
        wh[64 * z:64 * z + 64] = jnp.where(lane % 16 == z, spread, 0.0).astype(BF)

    def turned(value):
        return jnp.transpose(value.astype(F32)).astype(BF)

    def step(t, carry):
        for raw in (e_ref, j_ref):
            c = [raw[3 * t + k] for k in range(3)]
            o = jnp.zeros_like(c[0])
            for k, pair in enumerate(((c[0], o), (c[1], c[0]), (c[2], c[1]), (o, c[2]))):
                block = turned(jnp.concatenate(pair, axis=0))
                if raw is e_ref:
                    wb[pl.ds(pl.multiple_of(256 * t + 64 * k, 64), 64), :] = block
                else:
                    wj[t, k] = block
        for raw, out in ((m1_ref, w1), (m2_ref, w2)):
            for k in range(3):
                out[t, k] = turned(raw[3 * t + k])
        return carry

    for copy in copies[:4]:
        copy.wait()
    lax.fori_loop(0, 9, step, 0)
    copies[4].wait()
    for k in range(4):
        wu[:, 128 * k:128 * k + 128] = turned(jnp.concatenate([u_ref[2 * k], u_ref[2 * k + 1]], axis=0))


def weights(lift, encode, down, m1, m2, up, decode, head):
    shapes = ((2816, 128), (9, 3, 128, 128), (9, 3, 128, 128), (128, 512), (9, 4, 128, 128), (1024, 128))
    raw = (encode, m1, m2, up, decode)
    wb, w1, w2, wu, wj, wh = call(
        banded_kernel, (jnp.transpose(lift, (2, 0, 1)), head, jnp.asarray(LIFT_PICK, BF), *raw),
        [VM] * 3 + [HBM] * 5, [(shape, BF) for shape in shapes],
        [V(w.shape, BF) for w in raw] + [pltpu.SemaphoreType.DMA((5,))], limit=PREP, flops=6_000_000_000,
    )
    return wb, jnp.swapaxes(down, 1, 2).reshape(512, 128), w1, w2, wu, wj, wh


def quad_rows(blocks):
    o = jnp.zeros_like(blocks[0])
    columns = [[blocks[z - 2 * p + 1] if 0 <= z - 2 * p + 1 < 4 else o for z in (0, 1, 2, 3, 4, -1)] for p in range(2)]
    return jnp.concatenate([jnp.concatenate(c, axis=0) for c in columns], axis=1)


def pair_rows(blocks):
    o = jnp.zeros_like(blocks[0])
    columns = [[blocks[z - p] if 0 <= z - p < 3 else o for z in range(4)] for p in range(2)]
    return jnp.concatenate([jnp.concatenate(c, axis=0) for c in columns], axis=1)


def dot(a, b):
    return jnp.dot(a, b, preferred_element_type=F32)


def rows(parts):
    flat = [p.reshape(-1, p.shape[-1]) for p in parts]
    return flat[0] if len(flat) == 1 else jnp.concatenate(flat, axis=1)


def up_one(v):
    return pltpu.roll(v, v.shape[-2] - 1, v.ndim - 2)


def plane_kernel(d_ref, a_ref, top_ref, low_ref):
    for x in range(4):
        parts = [d_ref[k, x].astype(F32)[h:h + 8] for h in (8, 0) for k in range(3)]
        t = jnp.transpose(jnp.concatenate(parts, axis=0))
        t = jnp.concatenate([t, jnp.zeros((32, 80), F32)], axis=1)
        a_ref[x] = t.astype(BF)
        top_ref[x] = t[24:].astype(BF)
        low_ref[x] = t[:8].astype(BF)


def join_kernel(before_ref, a_ref, after_ref, o_ref):
    for x in range(4):
        parts = [r[x].astype(F32) for r in (before_ref, a_ref, after_ref)]
        o_ref[x] = jnp.concatenate(parts, axis=0).astype(BF)


def rim_kernel(b0, b1, b2, b3, b4, left_ref, right_ref):
    lane = lax.broadcasted_iota(jnp.int32, (16, 128), 1)
    for x in range(20):
        own = (b0, b1, b2, b3, b4)[x // 4][x % 4].astype(F32)
        for out, first in ((left_ref, 0), (right_ref, 24)):
            g = [own[16 * k:16 * k + 16] for k in range(3)]
            g = [t if 24 * k == first else pltpu.roll(t, (24 * k - first) % 128, 1) for k, t in enumerate(g)]
            out[x] = jnp.where(lane < 24, g[0], jnp.where(lane < 48, g[1], g[2])).astype(BF)


def tiles(df, dt):
    for yo in range(8):
        for xo in range(12):
            t = [df[pl.ds((8 * xi + xo) * 48 + yo, 8, stride=6), :] for xi in range(2)]
            dt[yo, xo] = jnp.concatenate(t, axis=0).astype(BF)


def lift(dt, wb_ref, db, fp, pairs, count, index):
    for one, two in pairs:
        table = pick((one, two))
        r = dot(rows([dt[b:b + 6] for b in range(3)]), table)
        r = r.astype(BF).reshape(6, 12, 16, 256)
        db[one] = r[..., :128]
        db[two] = r[..., 128:]
    first_slots = lax.broadcasted_iota(jnp.int32, (16, 128), 1) < 54

    def step(i, carry):
        q = index(i)
        for g in range(2):
            y = slice(3 * g, 3 * g + 3)
            ta = jnp.where(first_slots, db[q, y, 0:10], db[q, y, 1:11])
            table = jnp.concatenate([wb_ref[2304:2560], wb_ref[2560:2816]], axis=1)
            r = act(dot(rows([ta, db[q, y, 2:12]]), table))
            for half in range(2):
                part = r[:, 128 * half:128 * half + 128].reshape(3, 10, 16, 128)
                fp[2 * q + half, y] = part.astype(BF)
                if g == 0:
                    low_rows = part[0:2].reshape(40, 8, 128)
                    fp[2 * q + half, 6:8] = up_one(low_rows).reshape(2, 10, 16, 128).astype(BF)
        return carry

    lax.fori_loop(0, count, step, 0)


def encode(fp, fe, wb_ref, sk, sd, base, count, index):
    low = lax.broadcasted_iota(jnp.int32, (16, 128), 1) < 64

    def edge_step(i, carry):
        q = index(i)
        fe[q] = jnp.where(low, fp[2 * q + 3], fp[2 * q])
        return carry

    lax.fori_loop(0, count, edge_step, 0)

    def step(i, carry):
        q = index(i)
        for g in range(2):
            y0 = 3 * g
            acc = None
            for lo, hi in ENC:
                parts = []
                for t in range(lo, hi):
                    a, b = t // 3, t % 3
                    sl = (slice(y0 + b, y0 + b + 3), slice(a, a + 8))
                    parts += [fp[(2 * q + 1,) + sl], fp[(2 * q + 2,) + sl], fe[(q,) + sl]]
                p = dot(rows(parts), jnp.concatenate([quad_rows([wb_ref[256 * t + 64 * k:256 * t + 64 * k + 64] for k in range(4)]) for t in range(lo, hi)], axis=0))
                acc = p if acc is None else acc + p
            r = act(acc).reshape(3, 8, 2, 8, 256)
            for half in range(2):
                part = r[..., 128 * half:128 * half + 128]
                packed = part.reshape(3, 8, 16, 128).astype(BF)
                sp = 2 * q + half - base
                for yy in range(3):
                    yo = y0 + yy
                    sk[sp, yo // 2, yo % 2] = packed[yy].reshape(4, 2, 16, 128)
                    mixed = [jnp.concatenate([part[yy, (5 + xo) % 8, (5 + xo) // 8], part[yy, (7 + xo) % 8, (7 + xo) // 8]], axis=0)
                             for xo in range(4)]
                    mixed = jnp.stack(mixed).reshape(8, 8, 128)
                    if yo == 5:
                        sd[sp, 0] = mixed.reshape(4, 16, 128).astype(BF)
                    moved = up_one(mixed)
                    sd[sp, yo + 1] = moved.reshape(4, 16, 128).astype(BF)
                    if yo == 0:
                        sd[sp, 7] = up_one(moved).reshape(4, 16, 128).astype(BF)
        return carry

    lax.fori_loop(0, count, step, 0)


def inner_kernel(b0, b1, b2, b3, b4, wb_ref, sk, sd, df, dt, db, fp, fe):
    for k, ref in enumerate((b0, b1, b2, b3, b4)):
        for x in range(4):
            df[192 * k + 48 * x:192 * k + 48 * x + 48] = ref[x].astype(F32)
    df[960:968] = jnp.zeros((8, 128), F32)
    tiles(df, dt)
    lift(dt, wb_ref, db, fp, ((2, 3), (4, 5)), 4, lambda i: i + 2)
    encode(fp, fe, wb_ref, sk, sd, 4, 3, lambda i: i + 2)


def outer_kernel(b0, b1, b2, b3, b4, left_ref, right_ref, x_ref, wb_ref,
                 wd_ref, w1_ref, w2_ref, wu_ref, wj_ref, wh_ref, sk_in, sd_in, o_ref,
                 df, dt, db, fp, fe, sk, sd, c1, c2, de, uu, es, eu, hs, ac, sems):
    plan = ((sk_in, sk.at[4:10]), (sd_in, sd.at[4:10]))
    copies = [pltpu.make_async_copy(src, dst, sems.at[i]) for i, (src, dst) in enumerate(plan)]
    for copy in copies:
        copy.start()

    lane = lax.broadcasted_iota(jnp.int32, (16, 128), 1)
    low = lane < 64
    for x in range(20):
        own = (b0, b1, b2, b3, b4)[x // 4][x % 4].astype(F32)
        left, right = left_ref[x].astype(F32), right_ref[x].astype(F32)
        for g in range(3):
            t = jnp.where(lane < 72, pltpu.roll(left, 48 - 24 * g if g < 2 else 0, 1) if g < 2 else left,
                          pltpu.roll(right, 72 - 24 * g, 1))
            df[48 * x + 16 * g:48 * x + 16 * g + 16] = jnp.where(lane < 48, own[16 * g:16 * g + 16], t)
    df[960:968] = jnp.zeros((8, 128), F32)
    tiles(df, dt)
    lift(dt, wb_ref, db, fp, ((0, 1), (2, 5), (6, 7)), 6, lambda i: i + 2 * (i // 3))
    encode(fp, fe, wb_ref, sk, sd, 0, 4, lambda i: i + 3 * (i // 2))

    for copy in copies:
        copy.wait()
    r = act(dot(rows([sk[:, :, b, :, a] for a in range(2) for b in range(2)]), wd_ref[...]))
    r = r.reshape(7, 2, 3, 4, 2, 8, 128)
    for yo in range(3):
        for xo in range(5):
            t = jnp.stack([r[:, :, yo, xo % 4, xo // 4], r[:, :, yo, (3 + xo) % 4, (3 + xo) // 4]], axis=2)
            c1[:, :, yo, xo] = t.reshape(7, 2, 16, 128).astype(BF)
            if yo < 2:
                c1[:, :, yo + 3, xo] = up_one(t.reshape(28, 8, 128)).reshape(7, 2, 16, 128).astype(BF)

    def middle(src, w_ref, zp, xn):
        m = zp * xn * 48
        ac[:m] = jnp.zeros((m, 256), F32)

        def tap(a, carry):
            parts, table = [], []
            for b in range(3):
                parts += [src[zi // 2:zi // 2 + zp, zi % 2, b:b + 3, pl.ds(a, xn)] for zi in range(4)]
                table.append(pair_rows([w_ref[3 * a + b, k] for k in range(3)]))
            ac[:m] += dot(rows(parts), jnp.concatenate(table, axis=0))
            return carry

        lax.fori_loop(0, 3, tap, 0)
        return act(ac[:m]).reshape(zp, 3, xn, 2, 8, 256)

    r = middle(c1, w1_ref, 6, 3)
    for half in range(2):
        part = r[..., 128 * half:128 * half + 128]
        for yo in range(3):
            for xo in range(4):
                t = jnp.stack([part[:, yo, xo % 3, xo // 3], part[:, yo, (2 + xo) % 3, (2 + xo) // 3]], axis=1)
                c2[:, half, yo, xo] = t.reshape(6, 16, 128).astype(BF)
                if yo < 2:
                    c2[:, half, yo + 3, xo] = up_one(t.reshape(12, 8, 128)).reshape(6, 16, 128).astype(BF)

    r = middle(c2, w2_ref, 5, 2).reshape(5, 3, 2, 16, 256).astype(BF)
    de[:, 0] = r[..., :128]
    de[:, 1] = r[..., 128:]

    r = act(dot(rows([de[...]]), wu_ref[...])).reshape(5, 2, 3, 2, 2, 8, 512)
    for yo in range(6):
        b = yo % 2
        for xo in range(4):
            t = []
            for f in (1 + xo, 3 + xo):
                a = f % 2
                n = 128 * (2 * a + b)
                t.append(r[:, :, yo // 2, (f // 2) % 2, f // 4, :, n:n + 128])
            t = jnp.stack(t, axis=2)
            if yo > 0:
                uu[:, :, yo - 1, xo] = t.reshape(5, 2, 16, 128).astype(BF)
            if yo < 3:
                uu[:, :, yo + 5, xo] = up_one(t.reshape(20, 8, 128)).reshape(5, 2, 16, 128).astype(BF)

    for q in range(4):
        es[q] = jnp.where(low, sd[2 * q + 5], sd[2 * q + 2])
        eu[q] = jnp.where(low, uu[q + 1, 1], uu[q, 0])

    if True:
        ac[:768] = jnp.zeros((768, 256), F32)

        def tap(a, carry):
            parts, table = [], []
            for b in range(3):
                ys, xs, t = slice(b, b + 6), pl.ds(a, 2), 3 * a + b
                own = [jnp.stack([sd[2 * q + 3 + k, ys, xs] for q in range(4)]) for k in range(2)]
                parts += own + [es[:, ys, xs], uu[0:4, 1, ys, xs], uu[1:5, 0, ys, xs], eu[:, ys, xs]]
                blocks = [wj_ref[t, k] for k in range(4)]
                table += [quad_rows([w[:64] for w in blocks]), quad_rows([w[64:] for w in blocks])]
            ac[:768] += dot(rows(parts), jnp.concatenate(table, axis=0))
            return carry

        lax.fori_loop(0, 3, tap, 0)
        acc = ac[:768]
        j = act(acc).astype(BF).reshape(4, 192, 256)
        h = dot(jnp.concatenate([j[q] for q in range(4)], axis=1), wh_ref[...]).reshape(6, 2, 2, 8, 128)
        for yo in range(6):
            for x in range(4):
                hs[pl.ds(48 * x + yo, 8, stride=6), :] = h[yo, x % 2, x // 2]
    for x in range(4):
        t = jnp.transpose(hs[48 * x:48 * x + 32, :])
        for k in range(3):
            o_ref[k, x] = t[16 * k:16 * k + 16] + x_ref[k, x].astype(F32)


VM = pl.BlockSpec(memory_space=pltpu.VMEM)
HBM = pl.BlockSpec(memory_space=pltpu.HBM)


def call(body, args, specs, shapes, scratch=(), limit=16, flops=1_000_000):
    many = isinstance(shapes, list)
    return pl.pallas_call(
        body,
        out_shape=[jax.ShapeDtypeStruct(*x) for x in shapes] if many else jax.ShapeDtypeStruct(*shapes),
        in_specs=specs,
        out_specs=[VM] * len(shapes) if many else VM,
        scratch_shapes=scratch,
        compiler_params=pltpu.CompilerParams(vmem_limit_bytes=limit << 20),
        cost_estimate=pl.CostEstimate(flops=flops, bytes_accessed=2_000_000, transcendentals=0),
    )(*args)


def planes(d):
    return call(plane_kernel, (d,), [VM], [((4, 32, 128), BF), ((4, 8, 128), BF), ((4, 8, 128), BF)])


def rims(blocks):
    return call(rim_kernel, blocks, [VM] * 5, [((20, 16, 128), BF)] * 2, flops=4_000_000_000)


V = pltpu.VMEM
FIELDS = [V((968, 128), F32), V((8, 12, 16, 128), BF), V((8, 6, 12, 16, 128), BF), V((16, 8, 10, 16, 128), BF), V((7, 8, 10, 16, 128), BF)]
PREP, INNER, OUTER = 58, 20, 30
LIFT_PICK = lift_picker()


def inner(blocks, ws):
    args = (*blocks, ws[0])
    return call(
        inner_kernel, args, [VM] * 6, [((6, 3, 2, 4, 2, 16, 128), BF), ((6, 8, 4, 16, 128), BF)],
        FIELDS, limit=INNER, flops=8_000_000_000,
    )


def outer(blocks, left, right, d, ws, sk, sd):
    args = (*blocks, left, right, d, *ws, sk, sd)
    return call(
        outer_kernel, args, [VM] * 17, ((3, 4, 16, 32), F32),
        FIELDS + [
            V((14, 3, 2, 4, 2, 16, 128), BF), V((14, 8, 4, 16, 128), BF), V((7, 2, 5, 5, 16, 128), BF),
            V((6, 2, 5, 4, 16, 128), BF), V((5, 2, 3, 2, 16, 128), BF), V((5, 2, 8, 4, 16, 128), BF),
            V((4, 8, 4, 16, 128), BF), V((4, 8, 4, 16, 128), BF), V((200, 128), F32),
            V((864, 256), F32), pltpu.SemaphoreType.DMA((2,)),
        ], limit=OUTER, flops=16_000_000_000,
    )


def local(displacement, *raw):
    d = jnp.swapaxes(displacement, 2, 3)
    own, top, bottom = planes(d)
    before, after = shift(top, "gy", 1), shift(bottom, "gy", -1)
    ws = weights(*raw)
    block = call(join_kernel, (before, own, after), [VM] * 3, ((4, 48, 128), BF))
    blocks = (shift(block, "gx", 2), shift(block, "gx", 1), block, shift(block, "gx", -1), shift(block, "gx", -2))
    left, right = rims(blocks)
    left, right = shift(left, "gz", 1), shift(right, "gz", -1)
    sk, sd = inner(blocks, ws)
    return jnp.swapaxes(outer(blocks, left, right, d, ws, sk, sd), 2, 3)


def solution(mesh):
    placed = (P(None, "gx", "gy", "gz"), P(), P(), P(), P(), P(), P(), P(), P())
    return jax.shard_map(local, mesh=mesh, in_specs=placed, out_specs=P(None, "gx", "gy", "gz"), check_vma=False)
```
